256 devices in a mesh: half: 2 (over core), row: 16 (over x, y), col: 8 (over z).
Axes of the slice: x: 4, y: 4, z: 8, core: 2. Of those that a mesh axis runs over, the one named last changes fastest.
Arguments:
- particles: bfloat16 [512, 2, 64, 4096], P(('half', 'row', 'col')), may hold values from -9 to 9
- orient_bin: int32 [512], P(('half', 'row', 'col')), may hold values from 0 to 15
- tilt_slope: int32 [512, 2], P(('half', 'row', 'col')), may hold values from 12 to 40
- interp_table: bfloat16 [16, 3, 64, 64], replicated, may hold values from 0 to 1.6, as said below
Outputs:
- half_maps: float32 [2, 2, 64, 4096], P('half', None, 'row', 'col')
- shell_power: float32 [2, 29], replicated
- shell_correlation: float32 [2, 29], P('half')
The draws below stay inside these ranges and needn't reach their ends.
Inputs may be any that keep to these rules, and one draw needn't show every extreme that they name: `interp_table`: nonnegative entries.
All inputs are finite; a program needn't handle non-finite values.
Results may differ from the reference program's by a relative error of at most 0.00063.
Values sent between devices are 32-bit elements; how exact they have to be, the bound alone decides.
No kernel may reach another device: no remote copies, remote signals or barrier semaphores. Data moves between devices by JAX's collectives and lax.ppermute only.
A program may use at most 64 MiB of HBM per device.

```python
import jax
import jax.numpy as jnp
from jax import lax

GRID = 64
BINS = 16
SHELLS = 29
PARTICLES = 512


def draw_particles(key, part):
    full_shape = (PARTICLES, 2, GRID, GRID * GRID)
    signal = jax.random.normal(jax.random.fold_in(key, 11), (1, 2, GRID, GRID * GRID), jnp.float32)
    noise_part = jax.random.normal(key, full_shape, jnp.float32)
    combined = 0.7 * signal + noise_part
    return jnp.clip(combined, -9.0, 9.0).astype(jnp.bfloat16)


def draw_interp_table(key, part):
    full_shape = (BINS, 3, GRID, GRID)
    row_index = jnp.arange(GRID)[:, None]
    col_index = jnp.arange(GRID)[None, :]
    offset = jnp.abs(row_index - col_index)
    key_diagonal = jax.random.fold_in(key, 21)
    key_band = jax.random.fold_in(key, 22)
    key_dense = jax.random.fold_in(key, 23)
    diagonal_part = jax.random.uniform(key_diagonal, full_shape, jnp.float32, 0.8, 1.2)
    band_part = jax.random.uniform(key_band, full_shape, jnp.float32, 0.03, 0.25)
    dense_part = jax.random.uniform(key_dense, full_shape, jnp.float32, 0.0, 0.02)
    table = jnp.where(offset == 0, diagonal_part, jnp.where(offset <= 2, band_part, 0.0)) + dense_part
    return table.astype(jnp.bfloat16)


def set_ends(result, stream_key, least, high):
    index_at = [jax.random.randint(jax.random.fold_in(stream_key, axis), (), 0, length) for axis, length in enumerate(result.shape)]
    main_axis = result.shape.index(max(result.shape))
    beside = index_at[:main_axis] + [(index_at[main_axis] + 1) % result.shape[main_axis]] + index_at[main_axis + 1:]
    return result.at[tuple(index_at)].set(least).at[tuple(beside)].set(high)


def setup_inputs(seed: int = 0) -> dict:
    keys = jax.random.split(jax.random.key(seed), 5)
    particles = draw_particles(jax.random.fold_in(keys[4], 71), 0)
    orient_bin = set_ends(jax.random.randint(keys[1], (PARTICLES,), 0, BINS), jax.random.fold_in(keys[1], 1), 0, BINS - 1).astype(jnp.int32)
    tilt_slope = set_ends(jax.random.randint(keys[2], (PARTICLES, 2), 12, 41), jax.random.fold_in(keys[2], 1), 12, 40).astype(jnp.int32)
    interp_table = draw_interp_table(jax.random.fold_in(keys[4], 71), 0)
    return dict(particles=particles, orient_bin=orient_bin, tilt_slope=tilt_slope, interp_table=interp_table)


def wedge_mask(tilt_limits, grid_size):
    centre = grid_size // 2
    wave_first = (jnp.arange(grid_size, dtype=jnp.int32) - centre)[:, None]
    wave_third = (jnp.arange(grid_size * grid_size, dtype=jnp.int32) % grid_size - centre)[None, :]
    tilt_limit = jnp.where(wave_first * wave_third >= 0, tilt_limits[0], tilt_limits[1])
    inside = 16 * jnp.abs(wave_third) <= tilt_limit * jnp.abs(wave_first)
    return inside.astype(jnp.float32)

def interpolate(stacked, kernels, grid_size):
    components = stacked.shape[0]
    kernels = kernels.astype(jnp.float32)
    along_first = jnp.einsum('ax,cxm->cam', kernels[0], stacked.astype(jnp.float32), precision=lax.Precision.HIGHEST).astype(jnp.bfloat16)
    along_first = along_first.reshape(components, grid_size, grid_size, grid_size)
    along_second = jnp.einsum('by,cayz->cabz', kernels[1], along_first.astype(jnp.float32), precision=lax.Precision.HIGHEST).astype(jnp.bfloat16)
    along_third = jnp.einsum('dz,cabz->cabd', kernels[2], along_second.astype(jnp.float32), precision=lax.Precision.HIGHEST)
    return along_third.reshape(components, grid_size, grid_size * grid_size)

def reference(particles, orient_bin, tilt_slope, interp_table):
    grid_size = GRID
    half_labels = (jnp.arange(PARTICLES, dtype=jnp.int32) // (PARTICLES // 2)).astype(jnp.int32)

    def insert_one(partial_value, inputs):
        volume_data, bin_row, tilt_limits, half_label = inputs
        weight = wedge_mask(tilt_limits, grid_size)
        stacked = jnp.stack([volume_data[0] * weight, volume_data[1] * weight, weight]).astype(jnp.bfloat16)
        kernels = interp_table[bin_row]
        inserted = interpolate(stacked, kernels, grid_size)
        partial_value = partial_value.at[half_label].add(inserted)
        return (partial_value, None)
    partial_value = jnp.zeros((2, 3, grid_size, grid_size * grid_size), jnp.float32)
    partial_value, unused_out = lax.scan(insert_one, partial_value, (particles, orient_bin, tilt_slope, half_labels))
    half_maps = partial_value[:, :2] / (partial_value[:, 2:3] + 1.0)
    centre = grid_size // 2
    wave_first = (jnp.arange(grid_size, dtype=jnp.int32) - centre)[:, None]
    plane_index = jnp.arange(grid_size * grid_size, dtype=jnp.int32)[None, :]
    wave_second = plane_index // grid_size - centre
    wave_third = plane_index % grid_size - centre
    radius_sq = (wave_first * wave_first + wave_second * wave_second + wave_third * wave_third).reshape(-1)
    bounds = jnp.arange(4, centre, dtype=jnp.int32)
    shell_index = lax.optimization_barrier(jnp.sum((radius_sq[:, None] >= (bounds * bounds)[None, :]).astype(jnp.int32), axis=1)).astype(jnp.int32)
    shell_index = jnp.where(radius_sq < centre * centre, shell_index, SHELLS).astype(jnp.int32)
    map_first = half_maps[0]
    map_second = half_maps[1]
    cross_term = (map_first[0] * map_second[0] + map_first[1] * map_second[1]).reshape(-1)
    power_first = (map_first[0] * map_first[0] + map_first[1] * map_first[1]).reshape(-1)
    power_second = (map_second[0] * map_second[0] + map_second[1] * map_second[1]).reshape(-1)

    def shell_sum(values):
        return jax.ops.segment_sum(values, shell_index, num_segments=SHELLS + 1)[:SHELLS]
    cross_sum = shell_sum(cross_term)
    first_sum = shell_sum(power_first)
    second_sum = shell_sum(power_second)
    counts = shell_sum(jnp.ones_like(cross_term))
    shell_power = jnp.stack([first_sum, second_sum]) / counts[None, :]
    correlation = cross_sum / jnp.sqrt(first_sum * second_sum + 1e-06)
    shell_correlation = jnp.stack([correlation, correlation])
    return (half_maps, shell_power, shell_correlation)
```

```python
import functools

import jax
import jax.numpy as jnp
import numpy as np
from jax import lax
from jax.experimental import pallas as pl
from jax.experimental.pallas import tpu as pltpu
from jax.sharding import Mesh
from jax.sharding import PartitionSpec as P

SHELLS = 29
GRID = 64
CENTRE = GRID // 2
BINS = 16
ROWS = 16
COLS = 8
FIRST = GRID // ROWS
SECOND = GRID // COLS
SLOPE_MIN = 12
SLOPES = 29
PITCH = 72
BLOCK = FIRST * GRID
OWN = FIRST * SECOND
ROW = ("row_0", "row_1")
HALF_ROW_COL = ("half", "row_0", "row_1", "col")
F32 = jnp.float32
BF16 = jnp.bfloat16
VMEM = pl.BlockSpec(memory_space=pltpu.VMEM)
SMEM = pl.BlockSpec(memory_space=pltpu.SMEM)


def iota(shape, dim):
    return lax.broadcasted_iota(jnp.int32, shape, dim)


def wedge_tile(slope_first, slope_second):
    wave_first = iota((GRID, 128), 0) - CENTRE
    wave_third = iota((GRID, 128), 1) % GRID - CENTRE
    limit = jnp.where(wave_first * wave_third >= 0, slope_first, slope_second)
    inside = 16 * jnp.abs(wave_third) <= limit * jnp.abs(wave_first)
    return jnp.where(inside, 1.0, 0.0).astype(BF16)


def histogram_tile(bins, slopes):
    row, lane = iota((8, 128), 0), iota((8, 128), 1)
    total = jnp.zeros((8, 128), F32)
    for p in range(2):
        for quadrant in range(2):
            place = (bins[p] // 8) * 64 + quadrant * 32 + slopes[p, quadrant] - SLOPE_MIN
            total += jnp.where((row == bins[p] % 8) & (lane == place), 1.0, 0.0)
    return total


def insert_kernel(bins, slopes, particles, table, out, planes, third, chosen, sem):
    step = pl.program_id(0)

    @pl.when(step == 0)
    def _():
        copies = [
            pltpu.make_async_copy(table.at[bins[p]], chosen.at[p], sem.at[p]) for p in range(2)
        ]
        for copy in copies:
            copy.start()
        for copy in copies:
            copy.wait()
        third[...] = jnp.zeros_like(third)
        for p in range(2):
            transposed = chosen[p, 2].astype(F32).T.astype(BF16)
            for c in range(2):
                third[p * 128 + c * 64 : p * 128 + c * 64 + 64, c * 64 : c * 64 + 64] = transposed
        low = iota((GRID, 128), 1) < GRID
        for p in range(2):
            wedge = wedge_tile(slopes[p, 0], slopes[p, 1])
            wedge = jnp.concatenate([wedge] * 4, axis=1)
            first = chosen[p, 0]

            @pl.loop(0, 16, unroll=4)
            def _(chunk):
                lanes = pl.ds(pl.multiple_of(chunk * 256, 256), 256)
                volume = jnp.concatenate([particles[p, 0, :, lanes], particles[p, 1, :, lanes]], axis=1)
                along = jnp.dot(first, volume * wedge, preferred_element_type=F32)
                for j in range(2):
                    real = along[:, j * 128 : j * 128 + 128]
                    imag = along[:, 256 + j * 128 : 256 + j * 128 + 128]
                    even = jnp.where(low, real, pltpu.roll(imag, 64, 1))
                    odd = jnp.where(low, pltpu.roll(real, 64, 1), imag)
                    base = pl.multiple_of((chunk * 4 + j * 2) * PITCH, 8)
                    planes[p, pl.ds(base, GRID), :] = even
                    planes[p, pl.ds(base + PITCH, GRID), :] = odd

    for i in range(FIRST):
        parts = []
        for p in range(2):
            plane = planes[p, pl.ds(step * FIRST + i, GRID, stride=PITCH), :].astype(BF16)
            parts.append(jnp.dot(chosen[p, 1], plane, preferred_element_type=F32).astype(BF16))
        along = jnp.concatenate(parts, axis=1)
        full = jnp.dot(along, third[...], preferred_element_type=F32)
        for q in range(COLS):
            out[0, q * OWN + i * SECOND : q * OWN + (i + 1) * SECOND, :] = full[
                q * SECOND : (q + 1) * SECOND
            ]
    out[0, BLOCK : BLOCK + 8, :] = histogram_tile(bins, slopes)


def insert(particles, orient_bin, tilt_slope, table):
    return pl.pallas_call(
        insert_kernel,
        grid=(ROWS,),
        out_shape=jax.ShapeDtypeStruct((ROWS, BLOCK + 8, 128), F32),
        in_specs=[SMEM, SMEM, VMEM, pl.BlockSpec(memory_space=pl.ANY)],
        out_specs=pl.BlockSpec((1, BLOCK + 8, 128), lambda r: (r, 0, 0)),
        scratch_shapes=[
            pltpu.VMEM((2, GRID * PITCH, 128), F32),
            pltpu.VMEM((256, 128), BF16),
            pltpu.VMEM((2, 3, GRID, GRID), BF16),
            pltpu.SemaphoreType.DMA((2,)),
        ],
        compiler_params=pltpu.CompilerParams(vmem_limit_bytes=40 * 2**20),
        cost_estimate=pl.CostEstimate(flops=4 * 10**9, bytes_accessed=4 * 2**20, transcendentals=0),
        name="insert",
    )(orient_bin, tilt_slope, particles, table)


def row_sum_kernel(parts, out):
    total = parts[0]
    for k in range(1, ROWS):
        total = total + parts[k]
    for q in range(COLS):
        out[q, 0:OWN, :] = total[q * OWN : (q + 1) * OWN]
        out[q, OWN : OWN + 8, :] = total[BLOCK : BLOCK + 8]


def row_sum(parts):
    return pl.pallas_call(
        row_sum_kernel,
        out_shape=jax.ShapeDtypeStruct((COLS, OWN + 8, 128), F32),
        in_specs=[VMEM],
        out_specs=VMEM,
        name="row_sum",
    )(parts)


def quadrant_masks():
    shape = (GRID, SLOPES * 128)
    wave_first = iota(shape, 0) - CENTRE
    lane = iota(shape, 1)
    wave_third = lane % GRID - CENTRE
    quadrant = (lane // GRID) % 2
    slope = lane // 128 + SLOPE_MIN
    inside = 16 * jnp.abs(wave_third) <= slope * jnp.abs(wave_first)
    own = jnp.where(wave_first * wave_third >= 0, 0, 1) == quadrant
    return (inside & own).astype(BF16)


def spread_masks():
    shape = (128, SLOPES * 128)
    row, lane = iota(shape, 0), iota(shape, 1)
    return ((row % 32 == lane // 128) & ((row // 32) % 2 == (lane // GRID) % 2)).astype(BF16)


def divide_kernel(parts, grown, spread, second_sums, third, out, left):
    total = parts[0]
    for k in range(1, COLS):
        total = total + parts[k]
    counts = total[OWN : OWN + 8]
    low = iota((8, 128), 1) < GRID
    blocks = [jnp.where(low, counts, 0.0), jnp.where(low, 0.0, counts)] * FIRST
    counts = jnp.concatenate(blocks, axis=0).astype(BF16)
    held = jnp.zeros((FIRST * BINS, 128), F32)
    for k in range(SLOPES):
        lanes = slice(k * 128, k * 128 + 128)
        held += grown[:, lanes] * jnp.dot(counts, spread[:, lanes], preferred_element_type=F32)
    for k in range(BINS):
        sums = second_sums[k]
        for i in range(FIRST):
            value = sums * held[i * BINS + k : i * BINS + k + 1, :]
            upper = value.astype(BF16)
            left[i * SECOND : (i + 1) * SECOND, k * 128 : k * 128 + 128] = value
    value = left[...]
    upper = value.astype(BF16)
    lower = (value - upper.astype(F32)).astype(BF16)
    weight = jnp.dot(upper, third[...], preferred_element_type=F32)
    weight += jnp.dot(lower, third[...], preferred_element_type=F32)
    out[...] = total[0:OWN] / (weight + 1.0)


def divide(parts, grown, spread, second_sums, third):
    return pl.pallas_call(
        divide_kernel,
        out_shape=jax.ShapeDtypeStruct((OWN, 128), F32),
        in_specs=[VMEM] * 5,
        out_specs=VMEM,
        scratch_shapes=[pltpu.VMEM((OWN, BINS * 128), F32)],
        name="divide",
    )(parts, grown, spread, second_sums, third)


def spectra_kernel(place, own, other, out, rows):
    on_first = place[2] == 0
    a, b = own[...], other[...]
    cross = a * b
    own_power, other_power = a * a, b * b
    power_first = jnp.where(on_first, own_power, other_power)
    power_second = jnp.where(on_first, other_power, own_power)
    index = iota((OWN, 128), 0)
    first = index // SECOND + place[0] * FIRST - CENTRE
    second = index % SECOND + place[1] * SECOND - CENTRE
    third = iota((OWN, 128), 1) % GRID - CENTRE
    radius_sq = first * first + second * second + third * third
    rows[...] = jnp.zeros_like(rows)
    for k in range(SHELLS):
        least = 0 if k == 0 else (k + 3) ** 2
        inside = (radius_sq >= least) & (radius_sq < (k + 4) ** 2)
        for j, value in enumerate((cross, power_first, power_second)):
            rows[j * 32 + k : j * 32 + k + 1, :] = jnp.sum(
                jnp.where(inside, value, 0.0), axis=0, keepdims=True
            )
    rest = rows[...]
    ones = jnp.ones((8, 128), BF16)
    total = jnp.zeros((8, 128), F32)
    for _ in range(3):
        piece = rest.astype(BF16)
        rest = rest - piece.astype(F32)
        total += lax.dot_general(ones, piece, (((1,), (1,)), ((), ())), preferred_element_type=F32)
    for k in range(ROWS):
        out[k] = total


def spectra(place, own, other):
    return pl.pallas_call(
        spectra_kernel,
        out_shape=jax.ShapeDtypeStruct((ROWS, 8, 128), F32),
        in_specs=[SMEM, VMEM, VMEM],
        out_specs=VMEM,
        scratch_shapes=[pltpu.VMEM((128, 128), F32)],
        name="spectra",
    )(place, own, other)


def spread_kernel(parts, out):
    total = jnp.sum(parts[...], axis=0)
    for k in range(COLS):
        out[k] = total


def spread_sum(parts):
    return pl.pallas_call(
        spread_kernel,
        out_shape=jax.ShapeDtypeStruct((COLS, 8, 128), F32),
        in_specs=[VMEM],
        out_specs=VMEM,
        name="spread_sum",
    )(parts)


def finish_kernel(parts, counts, power, correlation):
    total = jnp.sum(parts[...], axis=0)
    cross = total[0:1, 0:SHELLS]
    first = total[0:1, 32 : 32 + SHELLS]
    second = total[0:1, 64 : 64 + SHELLS]
    power[0:1, :] = first / counts[...]
    power[1:2, :] = second / counts[...]
    correlation[...] = cross / jnp.sqrt(first * second + 1e-06)


def finish(parts, counts):
    return pl.pallas_call(
        finish_kernel,
        out_shape=(
            jax.ShapeDtypeStruct((2, SHELLS), F32),
            jax.ShapeDtypeStruct((1, SHELLS), F32),
        ),
        in_specs=[VMEM, VMEM],
        out_specs=(VMEM, VMEM),
        name="finish",
    )(parts, counts)


def shell_counts():
    wave = np.arange(GRID) - CENTRE
    radius_sq = (wave[:, None, None] ** 2 + wave[None, :, None] ** 2 + wave[None, None, :] ** 2).reshape(-1)
    bounds = np.arange(4, CENTRE) ** 2
    shell = np.searchsorted(bounds, radius_sq, side="right")
    inside = radius_sq < CENTRE * CENTRE
    return np.bincount(shell[inside], minlength=SHELLS).astype(np.float32)[None]


def local(particles, orient_bin, tilt_slope, table):
    row, col, half = lax.axis_index(ROW), lax.axis_index("col"), lax.axis_index("half")
    place = jnp.stack([row, col, half]).astype(jnp.int32)
    first = lax.dynamic_slice(table, (0, 0, row * FIRST, 0), (BINS, 1, FIRST, GRID))[:, 0]
    first = jnp.swapaxes(first, 0, 1).reshape(FIRST * BINS, GRID)
    grown = jnp.dot(first, quadrant_masks(), preferred_element_type=F32)
    second = lax.dynamic_slice(table, (0, 1, col * SECOND, 0), (BINS, 1, SECOND, GRID))[:, 0]
    second_sums = jnp.broadcast_to(
        jnp.sum(second.astype(F32), axis=2, keepdims=True), (BINS, SECOND, 128)
    )
    third = jnp.swapaxes(table[:, 2], 1, 2)
    third = jnp.broadcast_to(third[:, None, :, None, :], (BINS, 2, GRID, 2, GRID)).reshape(
        BINS * 128, 128
    )
    blocks = insert(particles, orient_bin, tilt_slope, table)
    parts = lax.all_to_all(blocks, ROW, 0, 0, tiled=True)
    blocks = row_sum(parts)
    parts = lax.all_to_all(blocks, "col", 0, 0, tiled=True)
    own = divide(parts, grown, spread_masks(), second_sums, third)
    other = lax.ppermute(own, "half", [(0, 1), (1, 0)])
    parts = lax.all_to_all(spectra(place, own, other), ROW, 0, 0, tiled=True)
    parts = lax.all_to_all(spread_sum(parts), "col", 0, 0, tiled=True)
    power, correlation = finish(parts, jnp.asarray(shell_counts()))
    half_maps = own.reshape(FIRST, SECOND, 2, GRID).transpose(2, 0, 1, 3)
    return half_maps.reshape(1, 2, FIRST, SECOND * GRID), power, correlation


def solution(mesh):
    torus = Mesh(
        mesh.devices.reshape(mesh.shape["half"], 4, 4, mesh.shape["col"]),
        ("half", "row_0", "row_1", "col"),
    )
    in_specs = (P(HALF_ROW_COL, None, None, None), P(HALF_ROW_COL), P(HALF_ROW_COL, None), P())
    out_specs = (P("half", None, ROW, "col"), P(), P("half", None))
    return jax.shard_map(local, mesh=torus, in_specs=in_specs, out_specs=out_specs, check_vma=False)
```

```python
import functools

import jax
import jax.numpy as jnp
import numpy as np
from jax import lax
from jax.experimental import pallas as pl
from jax.experimental.pallas import tpu as pltpu
from jax.sharding import Mesh
from jax.sharding import PartitionSpec as P

SHELLS = 29
GRID = 64
CENTRE = GRID // 2
BINS = 16
ROWS = 16
COLS = 8
FIRST = GRID // ROWS
SECOND = GRID // COLS
SLOPE_MIN = 12
SLOPES = 29
OWN = FIRST * SECOND
ROW = ("row_0", "row_1")
HALF_ROW_COL = ("half", "row_0", "row_1", "col")
F32 = jnp.float32
BF16 = jnp.bfloat16
VMEM = pl.BlockSpec(memory_space=pltpu.VMEM)
SMEM = pl.BlockSpec(memory_space=pltpu.SMEM)
ANY = pl.BlockSpec(memory_space=pl.ANY)
SMALL = pltpu.CompilerParams(vmem_limit_bytes=6 * 2**20)
PARTS = 1


def iota(shape, dim):
    return lax.broadcasted_iota(jnp.int32, shape, dim)


def wedge_tile(slope_first, slope_second):
    wave_first = iota((GRID, 128), 0) - CENTRE
    wave_third = iota((GRID, 128), 1) % GRID - CENTRE
    limit = jnp.where(wave_first * wave_third >= 0, slope_first, slope_second)
    inside = 16 * jnp.abs(wave_third) <= limit * jnp.abs(wave_first)
    return jnp.where(inside, 1.0, 0.0).astype(BF16)


def histogram_tile(bins, slopes):
    row, lane = iota((8, 128), 0), iota((8, 128), 1)
    total = jnp.zeros((8, 128), F32)
    for p in range(2):
        for quadrant in range(2):
            place = (bins[p] // 8) * 64 + quadrant * 32 + slopes[p, quadrant] - SLOPE_MIN
            total += jnp.where((row == bins[p] % 8) & (lane == place), 1.0, 0.0)
    return total


def insert_kernel(part, bins, slopes, particles, table, out, volume, planes, third, chosen, blocks, sem_in, sem_out):
    count = FIRST // PARTS
    height = ROWS * count
    pitch = height + 8
    tables = [
        pltpu.make_async_copy(table.at[bins[p]], chosen.at[p], sem_in.at[4 + p]) for p in range(2)
    ]
    volumes = [
        [
            pltpu.make_async_copy(particles.at[p, c], volume.at[p, c], sem_in.at[p * 2 + c])
            for c in range(2)
        ]
        for p in range(2)
    ]
    for copy in (*tables, *volumes[0], *volumes[1]):
        copy.start()
    third[...] = jnp.zeros_like(third)
    row = iota((height, GRID), 0)
    chosen_row = (row // count) * FIRST + part * count + row % count
    select = (iota((height, GRID), 1) == chosen_row).astype(BF16)
    wedges = [
        jnp.concatenate([wedge_tile(slopes[p, 0], slopes[p, 1])] * 4, axis=1) for p in range(2)
    ]
    for copy in tables:
        copy.wait()
    for p in range(2):
        transposed = chosen[p, 2].astype(F32).T.astype(BF16)
        for c in range(2):
            third[p * 128 + c * 64 : p * 128 + c * 64 + 64, c * 64 : c * 64 + 64] = transposed
    low = iota((height, 128), 1) < GRID
    for p in range(2):
        first = chosen[p, 0]
        if PARTS > 1:
            first = jnp.dot(select, first, preferred_element_type=F32).astype(BF16)
        for copy in volumes[p]:
            copy.wait()

        @pl.loop(0, 16, unroll=4)
        def _(chunk):
            lanes = pl.ds(pl.multiple_of(chunk * 256, 256), 256)
            both = jnp.concatenate([volume[p, 0, :, lanes], volume[p, 1, :, lanes]], axis=1)
            along = jnp.dot(first, both * wedges[p], preferred_element_type=F32)
            for j in range(2):
                real = along[:, j * 128 : j * 128 + 128]
                imag = along[:, 256 + j * 128 : 256 + j * 128 + 128]
                even = jnp.where(low, real, pltpu.roll(imag, 64, 1))
                odd = jnp.where(low, pltpu.roll(real, 64, 1), imag)
                base = pl.multiple_of((chunk * 4 + j * 2) * pitch, 8)
                planes[p, pl.ds(base, height), :] = even
                planes[p, pl.ds(base + pitch, height), :] = odd

    last = part == PARTS - 1
    size = COLS * count * SECOND
    if last:
        tile = histogram_tile(bins, slopes)
        for r in range(ROWS):
            blocks[r, size : size + 8, :] = tile
    group = 8 // count

    @pl.loop(0, ROWS // group)
    def _(step):
        for g in range(group):
            r = step * group + g
            for i in range(count):
                parts = []
                for p in range(2):
                    plane = planes[p, pl.ds(r * count + i, GRID, stride=pitch), :].astype(BF16)
                    along = jnp.dot(chosen[p, 1], plane, preferred_element_type=F32)
                    parts.append(along.astype(BF16))
                full = jnp.dot(
                    jnp.concatenate(parts, axis=1), third[...], preferred_element_type=F32
                )
                for q in range(COLS):
                    start = (q * count + i) * SECOND
                    blocks[r, start : start + SECOND, :] = full[q * SECOND : (q + 1) * SECOND]
        span = pl.ds(step * group, group)
        pltpu.make_async_copy(blocks.at[span], out.at[span], sem_out).start()

    pltpu.make_async_copy(blocks, out, sem_out).wait()


def insert(part, particles, orient_bin, tilt_slope, table):
    count = FIRST // PARTS
    rows = COLS * count * SECOND + (8 if part == PARTS - 1 else 0)
    return pl.pallas_call(
        functools.partial(insert_kernel, part),
        out_shape=jax.ShapeDtypeStruct((ROWS, rows, 128), F32),
        in_specs=[SMEM, SMEM, ANY, ANY],
        out_specs=ANY,
        scratch_shapes=[
            pltpu.VMEM((2, 2, GRID, GRID * GRID), BF16),
            pltpu.VMEM((2, GRID * (ROWS * count + 8), 128), F32),
            pltpu.VMEM((256, 128), BF16),
            pltpu.VMEM((2, 3, GRID, GRID), BF16),
            pltpu.VMEM((ROWS, rows, 128), F32),
            pltpu.SemaphoreType.DMA((6,)),
            pltpu.SemaphoreType.DMA,
        ],
        cost_estimate=pl.CostEstimate(flops=10**9, bytes_accessed=4 * 2**20, transcendentals=0),
        name=f"insert_{part}",
    )(orient_bin, tilt_slope, particles, table)


def row_sum_kernel(*refs):
    *parts, out = refs
    span = OWN // PARTS
    for n, part in enumerate(parts):
        total = part[0]
        for k in range(1, ROWS):
            total = total + part[k]
        for q in range(COLS):
            out[q, n * span : (n + 1) * span, :] = total[q * span : (q + 1) * span]
        if n == PARTS - 1:
            for q in range(COLS):
                out[q, OWN : OWN + 8, :] = total[COLS * span : COLS * span + 8]


def row_sum(*parts):
    return pl.pallas_call(
        row_sum_kernel,
        out_shape=jax.ShapeDtypeStruct((COLS, OWN + 8, 128), F32),
        in_specs=[VMEM] * len(parts),
        out_specs=VMEM,
        compiler_params=SMALL,
        name="row_sum",
    )(*parts)


def quadrant_masks():
    shape = (GRID, SLOPES * 128)
    wave_first = iota(shape, 0) - CENTRE
    lane = iota(shape, 1)
    wave_third = lane % GRID - CENTRE
    quadrant = (lane // GRID) % 2
    slope = lane // 128 + SLOPE_MIN
    inside = 16 * jnp.abs(wave_third) <= slope * jnp.abs(wave_first)
    own = jnp.where(wave_first * wave_third >= 0, 0, 1) == quadrant
    return (inside & own).astype(BF16)


def divide_kernel(parts, grown, second_sums, third, out, left):
    total = parts[0]
    for k in range(1, COLS):
        total = total + parts[k]
    counts = total[OWN : OWN + 8]
    low = iota((8, 128), 1) < GRID
    held = [[jnp.zeros((8, 128), F32) for _ in range(2)] for _ in range(FIRST)]
    for k in range(SLOPES):
        for upper in range(2):
            lane = upper * 64 + k
            spread = jnp.where(
                low,
                jnp.broadcast_to(counts[:, lane : lane + 1], (8, 128)),
                jnp.broadcast_to(counts[:, lane + 32 : lane + 33], (8, 128)),
            )
            for i in range(FIRST):
                start = i * BINS + upper * 8
                held[i][upper] += spread * grown[start : start + 8, k * 128 : k * 128 + 128]
    for k in range(BINS):
        sums = jnp.broadcast_to(second_sums[:, k : k + 1], (8, 128))
        for i in range(FIRST):
            value = sums * held[i][k // 8][k % 8 : k % 8 + 1, :]
            upper = value.astype(BF16)
            lower = (value - upper.astype(F32)).astype(BF16)
            lanes = slice(k * 128, k * 128 + 128)
            left[i * SECOND : (i + 1) * SECOND, lanes] = upper.astype(F32)
            left[OWN + i * SECOND : OWN + (i + 1) * SECOND, lanes] = lower.astype(F32)
    weight = jnp.dot(left[...].astype(BF16), third[...], preferred_element_type=F32)
    out[...] = total[0:OWN] / (weight[0:OWN] + weight[OWN:] + 1.0)


def divide(parts, grown, second_sums, third):
    return pl.pallas_call(
        divide_kernel,
        out_shape=jax.ShapeDtypeStruct((OWN, 128), F32),
        in_specs=[VMEM] * 4,
        out_specs=VMEM,
        scratch_shapes=[pltpu.VMEM((2 * OWN, BINS * 128), F32)],
        compiler_params=SMALL,
        name="divide",
    )(parts, grown, second_sums, third)


def spectra_kernel(own, other, out, maps, rows):
    on_first = lax.axis_index("half") == 0
    a, b = own[...], other[...]
    cross = a * b
    own_power, other_power = a * a, b * b
    power_first = jnp.where(on_first, own_power, other_power)
    power_second = jnp.where(on_first, other_power, own_power)
    index = iota((OWN, 128), 0)
    first = index // SECOND + lax.axis_index(ROW) * FIRST - CENTRE
    second = index % SECOND + lax.axis_index("col") * SECOND - CENTRE
    third = iota((OWN, 128), 1) % GRID - CENTRE
    radius_sq = first * first + second * second + third * third
    rows[...] = jnp.zeros_like(rows)
    for k in range(SHELLS):
        least = 0 if k == 0 else (k + 3) ** 2
        inside = (radius_sq >= least) & (radius_sq < (k + 4) ** 2)
        for j, value in enumerate((cross, power_first, power_second)):
            rows[j * 32 + k : j * 32 + k + 1, :] = jnp.sum(
                jnp.where(inside, value, 0.0), axis=0, keepdims=True
            )
    rest = rows[...]
    ones = jnp.ones((8, 128), BF16)
    total = jnp.zeros((8, 128), F32)
    for _ in range(3):
        piece = rest.astype(BF16)
        rest = rest - piece.astype(F32)
        total += lax.dot_general(ones, piece, (((1,), (1,)), ((), ())), preferred_element_type=F32)
    for k in range(ROWS):
        out[k] = total
    low = iota((SECOND // 2, 128), 1) < GRID
    for i in range(FIRST):
        even = own[pl.ds(i * SECOND, SECOND // 2, stride=2), :]
        odd = own[pl.ds(i * SECOND + 1, SECOND // 2, stride=2), :]
        real = jnp.where(low, even, pltpu.roll(odd, 64, 1))
        imag = jnp.where(low, pltpu.roll(even, 64, 1), odd)
        for j in range(SECOND // 2):
            lanes = slice(j * 128, j * 128 + 128)
            maps[0, 0, i : i + 1, lanes] = real[j : j + 1]
            maps[0, 1, i : i + 1, lanes] = imag[j : j + 1]


def spectra(own, other):
    return pl.pallas_call(
        spectra_kernel,
        out_shape=(
            jax.ShapeDtypeStruct((ROWS, 8, 128), F32),
            jax.ShapeDtypeStruct((1, 2, FIRST, SECOND * GRID), F32),
        ),
        in_specs=[VMEM, VMEM],
        out_specs=(VMEM, VMEM),
        scratch_shapes=[pltpu.VMEM((128, 128), F32)],
        compiler_params=SMALL,
        name="spectra",
    )(own, other)


def spread_kernel(parts, out):
    total = jnp.sum(parts[...], axis=0)
    for k in range(COLS):
        out[k] = total


def spread_sum(parts):
    return pl.pallas_call(
        spread_kernel,
        out_shape=jax.ShapeDtypeStruct((COLS, 8, 128), F32),
        in_specs=[VMEM],
        out_specs=VMEM,
        compiler_params=SMALL,
        name="spread_sum",
    )(parts)


def finish_kernel(parts, counts, power, correlation):
    total = jnp.sum(parts[...], axis=0)
    cross = total[0:1, 0:SHELLS]
    first = total[0:1, 32 : 32 + SHELLS]
    second = total[0:1, 64 : 64 + SHELLS]
    power[0:1, :] = first / counts[...]
    power[1:2, :] = second / counts[...]
    correlation[...] = cross / jnp.sqrt(first * second + 1e-06)


def finish(parts, counts):
    return pl.pallas_call(
        finish_kernel,
        out_shape=(
            jax.ShapeDtypeStruct((2, SHELLS), F32),
            jax.ShapeDtypeStruct((1, SHELLS), F32),
        ),
        in_specs=[VMEM, VMEM],
        out_specs=(VMEM, VMEM),
        compiler_params=SMALL,
        name="finish",
    )(parts, counts)


def shell_counts():
    wave = np.arange(GRID) - CENTRE
    radius_sq = (wave[:, None, None] ** 2 + wave[None, :, None] ** 2 + wave[None, None, :] ** 2).reshape(-1)
    bounds = np.arange(4, CENTRE) ** 2
    shell = np.searchsorted(bounds, radius_sq, side="right")
    inside = radius_sq < CENTRE * CENTRE
    return np.bincount(shell[inside], minlength=SHELLS).astype(np.float32)[None]


def local(particles, orient_bin, tilt_slope, table):
    row, col = lax.axis_index(ROW), lax.axis_index("col")
    first = lax.dynamic_slice(table, (0, 0, row * FIRST, 0), (BINS, 1, FIRST, GRID))[:, 0]
    first = jnp.swapaxes(first, 0, 1).reshape(FIRST * BINS, GRID)
    grown = jnp.dot(first, quadrant_masks(), preferred_element_type=F32)
    second = lax.dynamic_slice(table, (0, 1, col * SECOND, 0), (BINS, 1, SECOND, GRID))[:, 0]
    second_sums = jnp.sum(second.astype(F32), axis=2).T
    third = jnp.swapaxes(table[:, 2], 1, 2)
    third = jnp.broadcast_to(third[:, None, :, None, :], (BINS, 2, GRID, 2, GRID)).reshape(
        BINS * 128, 128
    )
    parts = []
    for n in range(PARTS):
        blocks = insert(n, particles, orient_bin, tilt_slope, table)
        parts.append(lax.all_to_all(blocks, ROW, 0, 0, tiled=True))
    parts, grown, second_sums, third = lax.optimization_barrier(
        (parts, grown, second_sums, third)
    )
    blocks = row_sum(*parts)
    parts = lax.all_to_all(blocks, "col", 0, 0, tiled=True)
    own = divide(parts, grown, second_sums, third)
    other = lax.ppermute(own, "half", [(0, 1), (1, 0)])
    sums, half_maps = spectra(own, other)
    parts = lax.all_to_all(sums, ROW, 0, 0, tiled=True)
    parts = lax.all_to_all(spread_sum(parts), "col", 0, 0, tiled=True)
    power, correlation = finish(parts, jnp.asarray(shell_counts()))
    return half_maps, power, correlation


def solution(mesh):
    torus = Mesh(
        mesh.devices.reshape(mesh.shape["half"], 4, 4, mesh.shape["col"]),
        ("half", "row_0", "row_1", "col"),
    )
    in_specs = (P(HALF_ROW_COL, None, None, None), P(HALF_ROW_COL), P(HALF_ROW_COL, None), P())
    out_specs = (P("half", None, ROW, "col"), P(), P("half", None))
    return jax.shard_map(local, mesh=torus, in_specs=in_specs, out_specs=out_specs, check_vma=False)
```

```python
import functools

import jax
import jax.numpy as jnp
import numpy as np
from jax import lax
from jax.experimental import pallas as pl
from jax.experimental.pallas import tpu as pltpu
from jax.sharding import Mesh
from jax.sharding import PartitionSpec as P

SHELLS = 29
GRID = 64
CENTRE = GRID // 2
BINS = 16
ROWS = 16
COLS = 8
FIRST = GRID // ROWS
SECOND = GRID // COLS
SLOPE_MIN = 12
SLOPES = 29
SIDE = 4
PITCH = 72
BLOCK = FIRST * GRID
OWN = FIRST * SECOND
ROW = ("row_0", "row_1")
HALF_ROW = ("half", "row_0", "row_1")
HALF_ROW_COL = ("half", "row_0", "row_1", "col")
F32 = jnp.float32
BF16 = jnp.bfloat16
VMEM = pl.BlockSpec(memory_space=pltpu.VMEM)
SMEM = pl.BlockSpec(memory_space=pltpu.SMEM)
ANY = pl.BlockSpec(memory_space=pl.ANY)
SMALL = pltpu.CompilerParams(vmem_limit_bytes=6 * 2**20)


def iota(shape, dim):
    return lax.broadcasted_iota(jnp.int32, shape, dim)


def wedge_tile(slope_first, slope_second):
    wave_first = iota((GRID, 128), 0) - CENTRE
    wave_third = iota((GRID, 128), 1) % GRID - CENTRE
    limit = jnp.where(wave_first * wave_third >= 0, slope_first, slope_second)
    inside = 16 * jnp.abs(wave_third) <= limit * jnp.abs(wave_first)
    return jnp.where(inside, 1.0, 0.0).astype(BF16)


def histogram_tile(bins, slopes):
    row, lane = iota((8, 128), 0), iota((8, 128), 1)
    total = jnp.zeros((8, 128), F32)
    for p in range(2):
        for quadrant in range(2):
            place = (bins[p] // 8) * 64 + quadrant * 32 + slopes[p, quadrant] - SLOPE_MIN
            total += jnp.where((row == bins[p] % 8) & (lane == place), 1.0, 0.0)
    return total


def insert_kernel(bins, slopes, particles, table, out, volume, planes, third, chosen, blocks, sem_in, sem_out):
    tables = [
        pltpu.make_async_copy(table.at[bins[p]], chosen.at[p], sem_in.at[4 + p]) for p in range(2)
    ]
    volumes = [
        [
            pltpu.make_async_copy(particles.at[p, c], volume.at[p, c], sem_in.at[p * 2 + c])
            for c in range(2)
        ]
        for p in range(2)
    ]
    for copy in (*tables, *volumes[0], *volumes[1]):
        copy.start()
    third[...] = jnp.zeros_like(third)
    wedges = [
        jnp.concatenate([wedge_tile(slopes[p, 0], slopes[p, 1])] * 4, axis=1) for p in range(2)
    ]
    counts = histogram_tile(bins, slopes)
    for k in range(SIDE):
        blocks[k, SIDE * BLOCK : SIDE * BLOCK + 8, :] = counts
    for copy in tables:
        copy.wait()
    for p in range(2):
        transposed = chosen[p, 2].astype(F32).T.astype(BF16)
        for c in range(2):
            third[p * 128 + c * 64 : p * 128 + c * 64 + 64, c * 64 : c * 64 + 64] = transposed
    low = iota((GRID, 128), 1) < GRID
    for p in range(2):
        for copy in volumes[p]:
            copy.wait()

        @pl.loop(0, 16, unroll=4)
        def _(chunk):
            lanes = pl.ds(pl.multiple_of(chunk * 256, 256), 256)
            both = jnp.concatenate([volume[p, 0, :, lanes], volume[p, 1, :, lanes]], axis=1)
            along = jnp.dot(chosen[p, 0], both * wedges[p], preferred_element_type=F32)
            for j in range(2):
                real = along[:, j * 128 : j * 128 + 128]
                imag = along[:, 256 + j * 128 : 256 + j * 128 + 128]
                even = jnp.where(low, real, pltpu.roll(imag, 64, 1))
                odd = jnp.where(low, pltpu.roll(real, 64, 1), imag)
                base = pl.multiple_of((chunk * 4 + j * 2) * PITCH, 8)
                planes[p, pl.ds(base, GRID), :] = even
                planes[p, pl.ds(base + PITCH, GRID), :] = odd

    on_first = lax.axis_index("half") == 0

    @pl.loop(0, ROWS // 2)
    def _(step):
        outer = step // 2
        for g in range(2):
            inner = (step % 2) * 2 + g
            row = jnp.where(on_first, outer * SIDE + inner, inner * SIDE + outer)
            for i in range(FIRST):
                parts = []
                for p in range(2):
                    plane = planes[p, pl.ds(row * FIRST + i, GRID, stride=PITCH), :].astype(BF16)
                    along = jnp.dot(chosen[p, 1], plane, preferred_element_type=F32)
                    parts.append(along.astype(BF16))
                full = jnp.dot(
                    jnp.concatenate(parts, axis=1), third[...], preferred_element_type=F32
                )
                for q in range(COLS):
                    start = inner * BLOCK + (q * FIRST + i) * SECOND
                    start = pl.multiple_of(start, 8)
                    blocks[outer, pl.ds(start, SECOND), :] = full[q * SECOND : (q + 1) * SECOND]

        @pl.when(step % 2 == 1)
        def _():
            pltpu.make_async_copy(blocks.at[outer], out.at[outer], sem_out).start()

    pltpu.make_async_copy(blocks, out, sem_out).wait()


def insert(particles, orient_bin, tilt_slope, table):
    rows = SIDE * BLOCK + 8
    return pl.pallas_call(
        insert_kernel,
        out_shape=jax.ShapeDtypeStruct((SIDE, rows, 128), F32),
        in_specs=[SMEM, SMEM, ANY, ANY],
        out_specs=ANY,
        scratch_shapes=[
            pltpu.VMEM((2, 2, GRID, GRID * GRID), BF16),
            pltpu.VMEM((2, GRID * PITCH, 128), F32),
            pltpu.VMEM((256, 128), BF16),
            pltpu.VMEM((2, 3, GRID, GRID), BF16),
            pltpu.VMEM((SIDE, rows, 128), F32),
            pltpu.SemaphoreType.DMA((6,)),
            pltpu.SemaphoreType.DMA,
        ],
        cost_estimate=pl.CostEstimate(flops=10**9, bytes_accessed=4 * 2**20, transcendentals=0),
        name="insert",
    )(orient_bin, tilt_slope, particles, table)


def reduce_kernel(owners, size, parts, out):
    senders = parts.shape[0]
    tail = pl.ds(owners * size, 8)
    counts = parts[0, tail, :]
    for k in range(1, senders):
        counts = counts + parts[k, tail, :]
    for n in range(owners):
        span = pl.ds(n * size, size)
        total = parts[0, span, :]
        for k in range(1, senders):
            total = total + parts[k, span, :]
        out[n, 0:size, :] = total
        out[n, size : size + 8, :] = counts


def reduce(parts, owners, size):
    return pl.pallas_call(
        functools.partial(reduce_kernel, owners, size),
        out_shape=jax.ShapeDtypeStruct((owners, size + 8, 128), F32),
        in_specs=[VMEM],
        out_specs=VMEM,
        compiler_params=SMALL,
        name=f"reduce_{owners}",
    )(parts)


def quadrant_masks():
    shape = (GRID, SLOPES * 128)
    wave_first = iota(shape, 0) - CENTRE
    lane = iota(shape, 1)
    wave_third = lane % GRID - CENTRE
    quadrant = (lane // GRID) % 2
    slope = lane // 128 + SLOPE_MIN
    inside = 16 * jnp.abs(wave_third) <= slope * jnp.abs(wave_first)
    own = jnp.where(wave_first * wave_third >= 0, 0, 1) == quadrant
    return (inside & own).astype(BF16)


def divide_kernel(parts, grown, second_sums, third, out, left):
    total = parts[0]
    for k in range(1, COLS):
        total = total + parts[k]
    counts = total[OWN : OWN + 8]
    low = iota((8, 128), 1) < GRID
    held = [[jnp.zeros((8, 128), F32) for _ in range(2)] for _ in range(FIRST)]
    for k in range(SLOPES):
        for upper in range(2):
            lane = upper * 64 + k
            spread = jnp.where(
                low,
                jnp.broadcast_to(counts[:, lane : lane + 1], (8, 128)),
                jnp.broadcast_to(counts[:, lane + 32 : lane + 33], (8, 128)),
            )
            for i in range(FIRST):
                start = i * BINS + upper * 8
                held[i][upper] += spread * grown[start : start + 8, k * 128 : k * 128 + 128]
    for k in range(BINS):
        sums = jnp.broadcast_to(second_sums[:, k : k + 1], (8, 128))
        for i in range(FIRST):
            value = sums * held[i][k // 8][k % 8 : k % 8 + 1, :]
            upper = value.astype(BF16)
            lower = (value - upper.astype(F32)).astype(BF16)
            lanes = slice(k * 128, k * 128 + 128)
            left[i * SECOND : (i + 1) * SECOND, lanes] = upper.astype(F32)
            left[OWN + i * SECOND : OWN + (i + 1) * SECOND, lanes] = lower.astype(F32)
    weight = jnp.dot(left[...].astype(BF16), third[...], preferred_element_type=F32)
    out[...] = total[0:OWN] / (weight[0:OWN] + weight[OWN:] + 1.0)


def divide(parts, grown, second_sums, third):
    return pl.pallas_call(
        divide_kernel,
        out_shape=jax.ShapeDtypeStruct((OWN, 128), F32),
        in_specs=[VMEM] * 4,
        out_specs=VMEM,
        scratch_shapes=[pltpu.VMEM((2 * OWN, BINS * 128), F32)],
        compiler_params=SMALL,
        name="divide",
    )(parts, grown, second_sums, third)


def spectra_kernel(own, other, out, maps, rows):
    on_first = lax.axis_index("half") == 0
    a, b = own[...], other[...]
    cross = a * b
    own_power, other_power = a * a, b * b
    power_first = jnp.where(on_first, own_power, other_power)
    power_second = jnp.where(on_first, other_power, own_power)
    index = iota((OWN, 128), 0)
    first = index // SECOND + lax.axis_index(ROW) * FIRST - CENTRE
    second = index % SECOND + lax.axis_index("col") * SECOND - CENTRE
    third = iota((OWN, 128), 1) % GRID - CENTRE
    radius_sq = first * first + second * second + third * third
    rows[...] = jnp.zeros_like(rows)
    for k in range(SHELLS):
        least = 0 if k == 0 else (k + 3) ** 2
        inside = (radius_sq >= least) & (radius_sq < (k + 4) ** 2)
        for j, value in enumerate((cross, power_first, power_second)):
            rows[j * 32 + k : j * 32 + k + 1, :] = jnp.sum(
                jnp.where(inside, value, 0.0), axis=0, keepdims=True
            )
    rest = rows[...]
    ones = jnp.ones((8, 128), BF16)
    total = jnp.zeros((8, 128), F32)
    for _ in range(3):
        piece = rest.astype(BF16)
        rest = rest - piece.astype(F32)
        total += lax.dot_general(ones, piece, (((1,), (1,)), ((), ())), preferred_element_type=F32)
    for k in range(ROWS):
        out[k] = total
    low = iota((SECOND // 2, 128), 1) < GRID
    for i in range(FIRST):
        even = own[pl.ds(i * SECOND, SECOND // 2, stride=2), :]
        odd = own[pl.ds(i * SECOND + 1, SECOND // 2, stride=2), :]
        real = jnp.where(low, even, pltpu.roll(odd, 64, 1))
        imag = jnp.where(low, pltpu.roll(even, 64, 1), odd)
        for j in range(SECOND // 2):
            lanes = slice(j * 128, j * 128 + 128)
            maps[0, 0, i : i + 1, lanes] = real[j : j + 1]
            maps[0, 1, i : i + 1, lanes] = imag[j : j + 1]


def spectra(own, other):
    return pl.pallas_call(
        spectra_kernel,
        out_shape=(
            jax.ShapeDtypeStruct((ROWS, 8, 128), F32),
            jax.ShapeDtypeStruct((1, 2, FIRST, SECOND * GRID), F32),
        ),
        in_specs=[VMEM, VMEM],
        out_specs=(VMEM, VMEM),
        scratch_shapes=[pltpu.VMEM((128, 128), F32)],
        compiler_params=SMALL,
        name="spectra",
    )(own, other)


def spread_kernel(parts, out):
    total = jnp.sum(parts[...], axis=0)
    for k in range(COLS):
        out[k] = total


def spread_sum(parts):
    return pl.pallas_call(
        spread_kernel,
        out_shape=jax.ShapeDtypeStruct((COLS, 8, 128), F32),
        in_specs=[VMEM],
        out_specs=VMEM,
        compiler_params=SMALL,
        name="spread_sum",
    )(parts)


def finish_kernel(parts, counts, power, correlation):
    total = jnp.sum(parts[...], axis=0)
    cross = total[0:1, 0:SHELLS]
    first = total[0:1, 32 : 32 + SHELLS]
    second = total[0:1, 64 : 64 + SHELLS]
    power[0:1, :] = first / counts[...]
    power[1:2, :] = second / counts[...]
    correlation[...] = cross / jnp.sqrt(first * second + 1e-06)


def finish(parts, counts):
    return pl.pallas_call(
        finish_kernel,
        out_shape=(
            jax.ShapeDtypeStruct((2, SHELLS), F32),
            jax.ShapeDtypeStruct((1, SHELLS), F32),
        ),
        in_specs=[VMEM, VMEM],
        out_specs=(VMEM, VMEM),
        compiler_params=SMALL,
        name="finish",
    )(parts, counts)


def groups(swapped):
    along_x = [[x * SIDE + y for x in range(SIDE)] for y in range(SIDE)]
    along_y = [[x * SIDE + y for y in range(SIDE)] for x in range(SIDE)]
    first, second = (along_y, along_x) if swapped else (along_x, along_y)
    return first + [[ROWS + k for k in group] for group in second]


def shell_counts():
    wave = np.arange(GRID) - CENTRE
    radius_sq = (wave[:, None, None] ** 2 + wave[None, :, None] ** 2 + wave[None, None, :] ** 2).reshape(-1)
    bounds = np.arange(4, CENTRE) ** 2
    shell = np.searchsorted(bounds, radius_sq, side="right")
    inside = radius_sq < CENTRE * CENTRE
    return np.bincount(shell[inside], minlength=SHELLS).astype(np.float32)[None]


def local(particles, orient_bin, tilt_slope, table):
    row, col = lax.axis_index(ROW), lax.axis_index("col")
    first = lax.dynamic_slice(table, (0, 0, row * FIRST, 0), (BINS, 1, FIRST, GRID))[:, 0]
    first = jnp.swapaxes(first, 0, 1).reshape(FIRST * BINS, GRID)
    grown = jnp.dot(first, quadrant_masks(), preferred_element_type=F32)
    second = lax.dynamic_slice(table, (0, 1, col * SECOND, 0), (BINS, 1, SECOND, GRID))[:, 0]
    second_sums = jnp.sum(second.astype(F32), axis=2).T
    third = jnp.swapaxes(table[:, 2], 1, 2)
    third = jnp.broadcast_to(third[:, None, :, None, :], (BINS, 2, GRID, 2, GRID)).reshape(
        BINS * 128, 128
    )
    blocks = insert(particles, orient_bin, tilt_slope, table)
    parts = lax.all_to_all(blocks, HALF_ROW, 0, 0, axis_index_groups=groups(False), tiled=True)
    parts, grown, second_sums, third = lax.optimization_barrier(
        (parts, grown, second_sums, third)
    )
    blocks = reduce(parts, SIDE, BLOCK)
    parts = lax.all_to_all(blocks, HALF_ROW, 0, 0, axis_index_groups=groups(True), tiled=True)
    blocks = reduce(parts, COLS, OWN)
    parts = lax.all_to_all(blocks, "col", 0, 0, tiled=True)
    own = divide(parts, grown, second_sums, third)
    other = lax.ppermute(own, "half", [(0, 1), (1, 0)])
    sums, half_maps = spectra(own, other)
    parts = lax.all_to_all(sums, ROW, 0, 0, tiled=True)
    parts = lax.all_to_all(spread_sum(parts), "col", 0, 0, tiled=True)
    power, correlation = finish(parts, jnp.asarray(shell_counts()))
    return half_maps, power, correlation


def solution(mesh):
    torus = Mesh(
        mesh.devices.reshape(mesh.shape["half"], 4, 4, mesh.shape["col"]),
        ("half", "row_0", "row_1", "col"),
    )
    in_specs = (P(HALF_ROW_COL, None, None, None), P(HALF_ROW_COL), P(HALF_ROW_COL, None), P())
    out_specs = (P("half", None, ROW, "col"), P(), P("half", None))
    return jax.shard_map(local, mesh=torus, in_specs=in_specs, out_specs=out_specs, check_vma=False)
```

```python
import functools

import jax
import jax.numpy as jnp
import numpy as np
from jax import lax
from jax.experimental import pallas as pl
from jax.experimental.pallas import tpu as pltpu
from jax.sharding import Mesh
from jax.sharding import PartitionSpec as P

SHELLS = 29
GRID = 64
CENTRE = GRID // 2
BINS = 16
ROWS = 16
COLS = 8
FIRST = GRID // ROWS
SECOND = GRID // COLS
SLOPE_MIN = 12
SLOPES = 29
SIDE = 4
PITCH = 72
BLOCK = FIRST * GRID
OWN = FIRST * SECOND
ROW = ("row_0", "row_1")
HALF_ROW = ("half", "row_0", "row_1")
HALF_ROW_COL = ("half", "row_0", "row_1", "col")
F32 = jnp.float32
BF16 = jnp.bfloat16
VMEM = pl.BlockSpec(memory_space=pltpu.VMEM)
HBM = pl.BlockSpec(memory_space=pltpu.HBM)
SMALL = pltpu.CompilerParams(vmem_limit_bytes=6 * 2**20)


def iota(shape, dim):
    return lax.broadcasted_iota(jnp.int32, shape, dim)


def wedge_tile(slope_first, slope_second):
    wave_first = iota((GRID, 128), 0) - CENTRE
    wave_third = iota((GRID, 128), 1) % GRID - CENTRE
    limit = jnp.where(wave_first * wave_third >= 0, slope_first, slope_second)
    inside = 16 * jnp.abs(wave_third) <= limit * jnp.abs(wave_first)
    return jnp.where(inside, 1.0, 0.0).astype(BF16)


def histogram_tile(bins, slopes):
    row, lane = iota((8, 128), 0), iota((8, 128), 1)
    total = jnp.zeros((8, 128), F32)
    for p in range(2):
        for quadrant in range(2):
            place = (bins[p] // 8) * 64 + quadrant * 32 + slopes[p, quadrant] - SLOPE_MIN
            total += jnp.where((row == bins[p] % 8) & (lane == place), 1.0, 0.0)
    return total


def compute_slab(shift, planes, second, third, counts, out):
    on_first = lax.axis_index("half") == 0
    mine = jnp.where(on_first, lax.axis_index("row_0"), lax.axis_index("row_1"))
    outer = lax.rem(mine + shift, SIDE)
    out[SIDE * BLOCK : SIDE * BLOCK + 8, :] = counts

    @pl.loop(0, SIDE // 2)
    def _(step):
        for g in range(2):
            inner = step * 2 + g
            row = jnp.where(on_first, outer * SIDE + inner, inner * SIDE + outer)
            for i in range(FIRST):
                parts = []
                for p in range(2):
                    plane = planes[p, pl.ds(row * FIRST + i, GRID, stride=PITCH), :].astype(BF16)
                    along = jnp.dot(second[p], plane, preferred_element_type=F32)
                    parts.append(along.astype(BF16))
                full = jnp.dot(
                    jnp.concatenate(parts, axis=1), third[...], preferred_element_type=F32
                )
                for q in range(COLS):
                    start = inner * BLOCK + (q * FIRST + i) * SECOND
                    start = pl.multiple_of(start, 8)
                    out[pl.ds(start, SECOND), :] = full[q * SECOND : (q + 1) * SECOND]


def first_kernel(bins_in, slopes_in, particles, table, planes, second, third, counts, out, volume, chosen, bins, slopes, sem):
    scalars = [
        pltpu.make_async_copy(bins_in, bins, sem.at[6]),
        pltpu.make_async_copy(slopes_in, slopes, sem.at[7]),
    ]
    volumes = [
        [
            pltpu.make_async_copy(particles.at[p, c], volume.at[p, c], sem.at[p * 2 + c])
            for c in range(2)
        ]
        for p in range(2)
    ]
    for copy in (*scalars, *volumes[0], *volumes[1]):
        copy.start()
    third[...] = jnp.zeros_like(third)
    for copy in scalars:
        copy.wait()
    tables = [
        pltpu.make_async_copy(table.at[bins[p]], chosen.at[p], sem.at[4 + p]) for p in range(2)
    ]
    for copy in tables:
        copy.start()
    wedges = [
        jnp.concatenate([wedge_tile(slopes[p, 0], slopes[p, 1])] * 4, axis=1) for p in range(2)
    ]
    counts[...] = histogram_tile(bins, slopes)
    for copy in tables:
        copy.wait()
    for p in range(2):
        second[p] = chosen[p, 1]
        transposed = chosen[p, 2].astype(F32).T.astype(BF16)
        for c in range(2):
            third[p * 128 + c * 64 : p * 128 + c * 64 + 64, c * 64 : c * 64 + 64] = transposed
    low = iota((GRID, 128), 1) < GRID
    for p in range(2):
        for copy in volumes[p]:
            copy.wait()

        @pl.loop(0, 16, unroll=4)
        def _(chunk):
            lanes = pl.ds(pl.multiple_of(chunk * 256, 256), 256)
            both = jnp.concatenate([volume[p, 0, :, lanes], volume[p, 1, :, lanes]], axis=1)
            along = jnp.dot(chosen[p, 0], both * wedges[p], preferred_element_type=F32)
            for j in range(2):
                real = along[:, j * 128 : j * 128 + 128]
                imag = along[:, 256 + j * 128 : 256 + j * 128 + 128]
                even = jnp.where(low, real, pltpu.roll(imag, 64, 1))
                odd = jnp.where(low, pltpu.roll(real, 64, 1), imag)
                base = pl.multiple_of((chunk * 4 + j * 2) * PITCH, 8)
                planes[p, pl.ds(base, GRID), :] = even
                planes[p, pl.ds(base + PITCH, GRID), :] = odd

    compute_slab(2, planes, second, third, counts[...], out)


SLAB = jax.ShapeDtypeStruct((SIDE * BLOCK + 8, 128), F32)


def first_slab(particles, orient_bin, tilt_slope, table):
    return pl.pallas_call(
        first_kernel,
        out_shape=(
            jax.ShapeDtypeStruct((2, GRID * PITCH, 128), F32),
            jax.ShapeDtypeStruct((2, GRID, GRID), BF16),
            jax.ShapeDtypeStruct((256, 128), BF16),
            jax.ShapeDtypeStruct((8, 128), F32),
            SLAB,
        ),
        in_specs=[HBM] * 4,
        out_specs=(VMEM,) * 5,
        scratch_shapes=[
            pltpu.VMEM((2, 2, GRID, GRID * GRID), BF16),
            pltpu.VMEM((2, 3, GRID, GRID), BF16),
            pltpu.SMEM((2,), jnp.int32),
            pltpu.SMEM((2, 2), jnp.int32),
            pltpu.SemaphoreType.DMA((8,)),
        ],
        compiler_params=pltpu.CompilerParams(vmem_limit_bytes=20 * 2**20),
        cost_estimate=pl.CostEstimate(flops=10**9, bytes_accessed=4 * 2**20, transcendentals=0),
        name="first_slab",
    )(orient_bin, tilt_slope, particles, table)


def slabs_kernel(planes, second, third, counts, *outs):
    for shift, out in zip((1, 3, 0), outs, strict=True):
        compute_slab(shift, planes, second, third, counts[...], out)


def other_slabs(planes, second, third, counts):
    return pl.pallas_call(
        slabs_kernel,
        out_shape=(SLAB,) * 3,
        in_specs=[VMEM] * 4,
        out_specs=(VMEM,) * 3,
        compiler_params=SMALL,
        cost_estimate=pl.CostEstimate(flops=10**9, bytes_accessed=2**20, transcendentals=0),
        name="other_slabs",
    )(planes, second, third, counts)


def gather_kernel(own, *refs):
    *others, out = refs
    tail = pl.ds(SIDE * BLOCK, 8)
    counts = own[tail, :]
    for other in others:
        counts = counts + other[tail, :]
    for n in range(SIDE):
        span = pl.ds(n * BLOCK, BLOCK)
        total = own[span, :]
        for other in others:
            total = total + other[span, :]
        out[n, 0:BLOCK, :] = total
        out[n, BLOCK : BLOCK + 8, :] = counts


def gather(*parts):
    return pl.pallas_call(
        gather_kernel,
        out_shape=jax.ShapeDtypeStruct((SIDE, BLOCK + 8, 128), F32),
        in_specs=[VMEM] * len(parts),
        out_specs=VMEM,
        compiler_params=SMALL,
        name="gather",
    )(*parts)


def reduce_kernel(owners, size, parts, out):
    senders = parts.shape[0]
    tail = pl.ds(owners * size, 8)
    counts = parts[0, tail, :]
    for k in range(1, senders):
        counts = counts + parts[k, tail, :]
    for n in range(owners):
        span = pl.ds(n * size, size)
        total = parts[0, span, :]
        for k in range(1, senders):
            total = total + parts[k, span, :]
        out[n, 0:size, :] = total
        out[n, size : size + 8, :] = counts


def reduce(parts, owners, size):
    return pl.pallas_call(
        functools.partial(reduce_kernel, owners, size),
        out_shape=jax.ShapeDtypeStruct((owners, size + 8, 128), F32),
        in_specs=[VMEM],
        out_specs=VMEM,
        compiler_params=SMALL,
    )(parts)


def quadrant_masks():
    shape = (GRID, SLOPES * 128)
    wave_first = iota(shape, 0) - CENTRE
    lane = iota(shape, 1)
    wave_third = lane % GRID - CENTRE
    quadrant = (lane // GRID) % 2
    slope = lane // 128 + SLOPE_MIN
    inside = 16 * jnp.abs(wave_third) <= slope * jnp.abs(wave_first)
    own = jnp.where(wave_first * wave_third >= 0, 0, 1) == quadrant
    return (inside & own).astype(BF16)


def divide_kernel(parts, grown, second_sums, third, out, left):
    total = parts[0]
    for k in range(1, COLS):
        total = total + parts[k]
    counts = total[OWN : OWN + 8]
    low = iota((8, 128), 1) < GRID
    held = [[jnp.zeros((8, 128), F32) for _ in range(2)] for _ in range(FIRST)]
    for k in range(SLOPES):
        for upper in range(2):
            lane = upper * 64 + k
            spread = jnp.where(
                low,
                jnp.broadcast_to(counts[:, lane : lane + 1], (8, 128)),
                jnp.broadcast_to(counts[:, lane + 32 : lane + 33], (8, 128)),
            )
            for i in range(FIRST):
                start = i * BINS + upper * 8
                held[i][upper] += spread * grown[start : start + 8, k * 128 : k * 128 + 128]
    for k in range(BINS):
        sums = jnp.broadcast_to(second_sums[:, k : k + 1], (8, 128))
        for i in range(FIRST):
            value = sums * held[i][k // 8][k % 8 : k % 8 + 1, :]
            upper = value.astype(BF16)
            lower = (value - upper.astype(F32)).astype(BF16)
            lanes = slice(k * 128, k * 128 + 128)
            left[i * SECOND : (i + 1) * SECOND, lanes] = upper.astype(F32)
            left[OWN + i * SECOND : OWN + (i + 1) * SECOND, lanes] = lower.astype(F32)
    weight = jnp.dot(left[...].astype(BF16), third[...], preferred_element_type=F32)
    out[...] = total[0:OWN] / (weight[0:OWN] + weight[OWN:] + 1.0)


def divide(parts, grown, second_sums, third):
    return pl.pallas_call(
        divide_kernel,
        out_shape=jax.ShapeDtypeStruct((OWN, 128), F32),
        in_specs=[VMEM] * 4,
        out_specs=VMEM,
        scratch_shapes=[pltpu.VMEM((2 * OWN, BINS * 128), F32)],
        compiler_params=SMALL,
        name="divide",
    )(parts, grown, second_sums, third)


def spectra_kernel(own, other, out, maps, rows):
    on_first = lax.axis_index("half") == 0
    a, b = own[...], other[...]
    cross = a * b
    own_power, other_power = a * a, b * b
    power_first = jnp.where(on_first, own_power, other_power)
    power_second = jnp.where(on_first, other_power, own_power)
    index = iota((OWN, 128), 0)
    first = index // SECOND + lax.axis_index(ROW) * FIRST - CENTRE
    second = index % SECOND + lax.axis_index("col") * SECOND - CENTRE
    third = iota((OWN, 128), 1) % GRID - CENTRE
    radius_sq = first * first + second * second + third * third
    rows[...] = jnp.zeros_like(rows)
    for k in range(SHELLS):
        least = 0 if k == 0 else (k + 3) ** 2
        inside = (radius_sq >= least) & (radius_sq < (k + 4) ** 2)
        for j, value in enumerate((cross, power_first, power_second)):
            rows[j * 32 + k : j * 32 + k + 1, :] = jnp.sum(
                jnp.where(inside, value, 0.0), axis=0, keepdims=True
            )
    rest = rows[...]
    ones = jnp.ones((8, 128), BF16)
    total = jnp.zeros((8, 128), F32)
    for _ in range(3):
        piece = rest.astype(BF16)
        rest = rest - piece.astype(F32)
        total += lax.dot_general(ones, piece, (((1,), (1,)), ((), ())), preferred_element_type=F32)
    for k in range(ROWS):
        out[k] = total
    low = iota((SECOND // 2, 128), 1) < GRID
    for i in range(FIRST):
        even = own[pl.ds(i * SECOND, SECOND // 2, stride=2), :]
        odd = own[pl.ds(i * SECOND + 1, SECOND // 2, stride=2), :]
        real = jnp.where(low, even, pltpu.roll(odd, 64, 1))
        imag = jnp.where(low, pltpu.roll(even, 64, 1), odd)
        for j in range(SECOND // 2):
            lanes = slice(j * 128, j * 128 + 128)
            maps[0, 0, i : i + 1, lanes] = real[j : j + 1]
            maps[0, 1, i : i + 1, lanes] = imag[j : j + 1]


def spectra(own, other):
    return pl.pallas_call(
        spectra_kernel,
        out_shape=(
            jax.ShapeDtypeStruct((ROWS, 8, 128), F32),
            jax.ShapeDtypeStruct((1, 2, FIRST, SECOND * GRID), F32),
        ),
        in_specs=[VMEM, VMEM],
        out_specs=(VMEM, VMEM),
        scratch_shapes=[pltpu.VMEM((128, 128), F32)],
        compiler_params=SMALL,
        name="spectra",
    )(own, other)


def spread_kernel(parts, out):
    total = jnp.sum(parts[...], axis=0)
    for k in range(COLS):
        out[k] = total


def spread_sum(parts):
    return pl.pallas_call(
        spread_kernel,
        out_shape=jax.ShapeDtypeStruct((COLS, 8, 128), F32),
        in_specs=[VMEM],
        out_specs=VMEM,
        compiler_params=SMALL,
        name="spread_sum",
    )(parts)


def finish_kernel(parts, counts, power, correlation):
    total = jnp.sum(parts[...], axis=0)
    cross = total[0:1, 0:SHELLS]
    first = total[0:1, 32 : 32 + SHELLS]
    second = total[0:1, 64 : 64 + SHELLS]
    power[0:1, :] = first / counts[...]
    power[1:2, :] = second / counts[...]
    correlation[...] = cross / jnp.sqrt(first * second + 1e-06)


def finish(parts, counts):
    return pl.pallas_call(
        finish_kernel,
        out_shape=(
            jax.ShapeDtypeStruct((2, SHELLS), F32),
            jax.ShapeDtypeStruct((1, SHELLS), F32),
        ),
        in_specs=[VMEM, VMEM],
        out_specs=(VMEM, VMEM),
        compiler_params=SMALL,
        name="finish",
    )(parts, counts)


def groups():
    along_x = [[x * SIDE + y for x in range(SIDE)] for y in range(SIDE)]
    along_y = [[x * SIDE + y for y in range(SIDE)] for x in range(SIDE)]
    return along_y + [[ROWS + k for k in group] for group in along_x]


def shifted(shift):
    pairs = []
    for x in range(SIDE):
        for y in range(SIDE):
            source = x * SIDE + y
            pairs.append((source, (x + shift) % SIDE * SIDE + y))
            pairs.append((ROWS + source, ROWS + x * SIDE + (y + shift) % SIDE))
    return pairs


def shell_counts():
    wave = np.arange(GRID) - CENTRE
    radius_sq = (wave[:, None, None] ** 2 + wave[None, :, None] ** 2 + wave[None, None, :] ** 2).reshape(-1)
    bounds = np.arange(4, CENTRE) ** 2
    shell = np.searchsorted(bounds, radius_sq, side="right")
    inside = radius_sq < CENTRE * CENTRE
    return np.bincount(shell[inside], minlength=SHELLS).astype(np.float32)[None]


def local(particles, orient_bin, tilt_slope, table):
    row, col = lax.axis_index(ROW), lax.axis_index("col")
    first = lax.dynamic_slice(table, (0, 0, row * FIRST, 0), (BINS, 1, FIRST, GRID))[:, 0]
    first = jnp.swapaxes(first, 0, 1).reshape(FIRST * BINS, GRID)
    grown = jnp.dot(first, quadrant_masks(), preferred_element_type=F32)
    second = lax.dynamic_slice(table, (0, 1, col * SECOND, 0), (BINS, 1, SECOND, GRID))[:, 0]
    second_sums = jnp.sum(second.astype(F32), axis=2).T
    third = jnp.swapaxes(table[:, 2], 1, 2)
    third = jnp.broadcast_to(third[:, None, :, None, :], (BINS, 2, GRID, 2, GRID)).reshape(
        BINS * 128, 128
    )
    inputs = [
        pltpu.with_memory_space_constraint(x, pltpu.HBM)
        for x in (particles, orient_bin, tilt_slope, table)
    ]
    *held, far = first_slab(*inputs)
    far = lax.ppermute(far, HALF_ROW, shifted(2))
    after, before, own = other_slabs(*held)
    after = lax.ppermute(after, HALF_ROW, shifted(1))
    before = lax.ppermute(before, HALF_ROW, shifted(3))
    parts = [own, after, before, far]
    parts, grown, second_sums, third = lax.optimization_barrier(
        (parts, grown, second_sums, third)
    )
    blocks = gather(*parts)
    parts = lax.all_to_all(blocks, HALF_ROW, 0, 0, axis_index_groups=groups(), tiled=True)
    blocks = reduce(parts, COLS, OWN)
    parts = lax.all_to_all(blocks, "col", 0, 0, tiled=True)
    own = divide(parts, grown, second_sums, third)
    other = lax.ppermute(own, "half", [(0, 1), (1, 0)])
    sums, half_maps = spectra(own, other)
    parts = lax.all_to_all(sums, ROW, 0, 0, tiled=True)
    parts = lax.all_to_all(spread_sum(parts), "col", 0, 0, tiled=True)
    power, correlation = finish(parts, jnp.asarray(shell_counts()))
    return half_maps, power, correlation


def solution(mesh):
    torus = Mesh(
        mesh.devices.reshape(mesh.shape["half"], 4, 4, mesh.shape["col"]),
        ("half", "row_0", "row_1", "col"),
    )
    in_specs = (P(HALF_ROW_COL, None, None, None), P(HALF_ROW_COL), P(HALF_ROW_COL, None), P())
    out_specs = (P("half", None, ROW, "col"), P(), P("half", None))
    return jax.shard_map(local, mesh=torus, in_specs=in_specs, out_specs=out_specs, check_vma=False)
```

```python
import jax
import jax.numpy as jnp
import numpy as np
from jax import lax
from jax.experimental import pallas as pl
from jax.experimental.pallas import tpu as pltpu
from jax.sharding import Mesh
from jax.sharding import PartitionSpec as P

SHELLS = 29
GRID = 64
CENTRE = GRID // 2
BINS = 16
ROWS = 16
COLS = 8
FIRST = GRID // ROWS
SECOND = GRID // COLS
SLOPE_MIN = 12
SLOPES = 29
SIDE = 4
PITCH = 68
BLOCK = FIRST * GRID
OWN = FIRST * SECOND
ROW = ("row_0", "row_1")
HALF_ROW = ("half", "row_0", "row_1")
HALF_ROW_COL = ("half", "row_0", "row_1", "col")
F32 = jnp.float32
BF16 = jnp.bfloat16
VMEM = pl.BlockSpec(memory_space=pltpu.VMEM)
HBM = pl.BlockSpec(memory_space=pltpu.HBM)
SMALL = pltpu.CompilerParams(vmem_limit_bytes=6 * 2**20)


def iota(shape, dim):
    return lax.broadcasted_iota(jnp.int32, shape, dim)


def wedge_tile(slope_first, slope_second):
    wave_first = iota((GRID, 128), 0) - CENTRE
    wave_third = iota((GRID, 128), 1) % GRID - CENTRE
    limit = jnp.where(wave_first * wave_third >= 0, slope_first, slope_second)
    inside = 16 * jnp.abs(wave_third) <= limit * jnp.abs(wave_first)
    return jnp.where(inside, 1.0, 0.0).astype(BF16)


def histogram_tile(bins, slopes):
    row, lane = iota((8, 128), 0), iota((8, 128), 1)
    total = jnp.zeros((8, 128), F32)
    for p in range(2):
        for quadrant in range(2):
            place = (bins[p] // 8) * 64 + quadrant * 32 + slopes[p, quadrant] - SLOPE_MIN
            total += jnp.where((row == bins[p] % 8) & (lane == place), 1.0, 0.0)
    return total


def compute_slab(shift, inners, planes, second, third, out, counts=None):
    on_first = lax.axis_index("half") == 0
    mine = jnp.where(on_first, lax.axis_index("row_0"), lax.axis_index("row_1"))
    outer = lax.rem(mine + shift, SIDE)
    for n, inner in enumerate(inners):
        row = jnp.where(on_first, outer * SIDE + inner, inner * SIDE + outer)
        for i in range(FIRST):
            parts = []
            for p in range(2):
                plane = planes[p, pl.ds(row * FIRST + i, GRID, stride=PITCH), :].astype(BF16)
                along = jnp.dot(second[p], plane, preferred_element_type=F32)
                parts.append(along.astype(BF16))
            full = jnp.dot(jnp.concatenate(parts, axis=1), third[...], preferred_element_type=F32)
            for q in range(COLS):
                start = n * BLOCK + (q * FIRST + i) * SECOND
                out[start : start + SECOND, :] = full[q * SECOND : (q + 1) * SECOND]
    if counts is not None:
        out[len(inners) * BLOCK : len(inners) * BLOCK + 8, :] = counts[...]


LOW = (0, 1)
HIGH = (2, 3)
HALF_SLAB = jax.ShapeDtypeStruct((2 * BLOCK, 128), F32)
HALF_SLAB_COUNTS = jax.ShapeDtypeStruct((2 * BLOCK + 8, 128), F32)
SLAB = jax.ShapeDtypeStruct((SIDE * BLOCK + 8, 128), F32)


def first_kernel(bins_in, slopes_in, particles, table, planes, second, third, counts, far_low, far_high, volume, chosen, bins, slopes, sem):
    scalars = [
        pltpu.make_async_copy(bins_in, bins, sem.at[6]),
        pltpu.make_async_copy(slopes_in, slopes, sem.at[7]),
    ]
    volumes = [
        pltpu.make_async_copy(
            particles.at[:, :, :, pl.ds(k * 1024, 1024)],
            volume.at[:, :, :, pl.ds(k * 1024, 1024)],
            sem.at[k],
        )
        for k in range(4)
    ]
    for copy in (*scalars, volumes[0]):
        copy.start()
    third[...] = jnp.zeros_like(third)
    low = iota((GRID, 128), 1) < GRID
    for copy in scalars:
        copy.wait()
    tables = [
        pltpu.make_async_copy(table.at[bins[p]], chosen.at[p], sem.at[4 + p]) for p in range(2)
    ]
    for copy in (*tables, *volumes[1:]):
        copy.start()
    wedges = [
        jnp.concatenate([wedge_tile(slopes[p, 0], slopes[p, 1])] * 4, axis=1) for p in range(2)
    ]
    counts[...] = histogram_tile(bins, slopes)
    for copy in tables:
        copy.wait()
    for p in range(2):
        second[p] = chosen[p, 1]
        transposed = chosen[p, 2].astype(F32).T.astype(BF16)
        for c in range(2):
            third[p * 128 + c * 64 : p * 128 + c * 64 + 64, c * 64 : c * 64 + 64] = transposed
    first = [chosen[p, 0] for p in range(2)]

    def transform(chunk):
        lanes = pl.ds(pl.multiple_of(chunk * 256, 256), 256)
        for p in range(2):
            both = jnp.concatenate([volume[p, 0, :, lanes], volume[p, 1, :, lanes]], axis=1)
            along = jnp.dot(first[p], both * wedges[p], preferred_element_type=F32)
            for j in range(2):
                real = along[:, j * 128 : j * 128 + 128]
                imag = along[:, 256 + j * 128 : 256 + j * 128 + 128]
                even = jnp.where(low, real, pltpu.roll(imag, 64, 1))
                odd = jnp.where(low, pltpu.roll(real, 64, 1), imag)
                base = pl.multiple_of((chunk * 4 + j * 2) * PITCH, 4)
                planes[p, pl.ds(base, GRID), :] = even
                planes[p, pl.ds(base + PITCH, GRID), :] = odd

    for k in range(4):
        volumes[k].wait()

        @pl.loop(k * 4, k * 4 + 4, unroll=4)
        def _(chunk):
            transform(chunk)

    compute_slab(2, LOW, planes, second, third, far_low, counts)
    compute_slab(2, HIGH, planes, second, third, far_high)


def first_slab(particles, orient_bin, tilt_slope, table):
    return pl.pallas_call(
        first_kernel,
        out_shape=(
            jax.ShapeDtypeStruct((2, GRID * PITCH, 128), F32),
            jax.ShapeDtypeStruct((2, GRID, GRID), BF16),
            jax.ShapeDtypeStruct((256, 128), BF16),
            jax.ShapeDtypeStruct((8, 128), F32),
            HALF_SLAB_COUNTS,
            HALF_SLAB,
        ),
        in_specs=[HBM] * 4,
        out_specs=(VMEM,) * 6,
        scratch_shapes=[
            pltpu.VMEM((2, 2, GRID, GRID * GRID), BF16),
            pltpu.VMEM((2, 3, GRID, GRID), BF16),
            pltpu.SMEM((2,), jnp.int32),
            pltpu.SMEM((2, 2), jnp.int32),
            pltpu.SemaphoreType.DMA((8,)),
        ],
        compiler_params=pltpu.CompilerParams(vmem_limit_bytes=20 * 2**20),
        cost_estimate=pl.CostEstimate(flops=10**9, bytes_accessed=4 * 2**20, transcendentals=0),
        name="first_slab",
    )(orient_bin, tilt_slope, particles, table)


def direct_kernel(planes, second, third, counts, after_high, before_low):
    compute_slab(1, HIGH, planes, second, third, after_high)
    compute_slab(3, LOW, planes, second, third, before_low, counts)


def direct_slabs(planes, second, third, counts):
    return pl.pallas_call(
        direct_kernel,
        out_shape=(HALF_SLAB, HALF_SLAB_COUNTS),
        in_specs=[VMEM] * 4,
        out_specs=(VMEM,) * 2,
        compiler_params=SMALL,
        cost_estimate=pl.CostEstimate(flops=10**9, bytes_accessed=2**20, transcendentals=0),
        name="direct_slabs",
    )(planes, second, third, counts)


def other_kernel(planes, second, third, counts, after_low, before_high, own):
    compute_slab(1, LOW, planes, second, third, after_low, counts)
    compute_slab(3, HIGH, planes, second, third, before_high)
    compute_slab(0, LOW + HIGH, planes, second, third, own, counts)


def other_slabs(planes, second, third, counts):
    return pl.pallas_call(
        other_kernel,
        out_shape=(HALF_SLAB_COUNTS, HALF_SLAB, SLAB),
        in_specs=[VMEM] * 4,
        out_specs=(VMEM,) * 3,
        compiler_params=SMALL,
        cost_estimate=pl.CostEstimate(flops=10**9, bytes_accessed=2**20, transcendentals=0),
        name="other_slabs",
    )(planes, second, third, counts)


def add_kernel(after_low, far_low, before_high, far_high, after_out, before_out):
    after_out[...] = after_low[...] + far_low[...]
    before_out[...] = before_high[...] + far_high[...]


def add_far(after_low, far_low, before_high, far_high):
    return pl.pallas_call(
        add_kernel,
        out_shape=(HALF_SLAB_COUNTS, HALF_SLAB),
        in_specs=[VMEM] * 4,
        out_specs=(VMEM,) * 2,
        compiler_params=SMALL,
        cost_estimate=pl.CostEstimate(flops=10**8, bytes_accessed=2**20, transcendentals=0),
        name="add_far",
    )(after_low, far_low, before_high, far_high)


def gather_kernel(own, after_low, after_high, before_low, before_high, *refs):
    *outs, sums = refs
    on_first = lax.axis_index("half") == 0
    mine = jnp.where(on_first, lax.axis_index("row_1"), lax.axis_index("row_0"))
    half = 2 * BLOCK
    tail = pl.ds(half, 8)
    counts = own[pl.ds(2 * half, 8), :] + after_low[tail, :] + before_low[tail, :]
    for n, parts in enumerate(((after_low, before_low), (after_high, before_high))):
        span = pl.ds(n * half, half)
        sums[span, :] = own[span, :] + parts[0][0:half, :] + parts[1][0:half, :]
    for shift, out in zip((2, 1, 3, 0), outs, strict=True):
        span = pl.ds(pl.multiple_of(lax.rem(mine + shift, SIDE) * BLOCK, 8), BLOCK)
        out[0:BLOCK, :] = sums[span, :]
        out[BLOCK : BLOCK + 8, :] = counts


def gather(*parts):
    return pl.pallas_call(
        gather_kernel,
        out_shape=(jax.ShapeDtypeStruct((BLOCK + 8, 128), F32),) * SIDE,
        in_specs=[VMEM] * len(parts),
        out_specs=(VMEM,) * SIDE,
        scratch_shapes=[pltpu.VMEM((SIDE * BLOCK, 128), F32)],
        compiler_params=SMALL,
        name="gather",
    )(*parts)


def reduce_kernel(*refs):
    *parts, out = refs
    tail = pl.ds(BLOCK, 8)
    counts = parts[0][tail, :]
    for part in parts[1:]:
        counts = counts + part[tail, :]
    for n in range(COLS):
        span = pl.ds(n * OWN, OWN)
        total = parts[0][span, :]
        for part in parts[1:]:
            total = total + part[span, :]
        out[n, 0:OWN, :] = total
        out[n, OWN : OWN + 8, :] = counts


def reduce(*parts):
    return pl.pallas_call(
        reduce_kernel,
        out_shape=jax.ShapeDtypeStruct((COLS, OWN + 8, 128), F32),
        in_specs=[VMEM] * len(parts),
        out_specs=VMEM,
        compiler_params=SMALL,
        name="reduce",
    )(*parts)


def operators_kernel(table, third, grown, second_sums, first):
    row, col = lax.axis_index(ROW), lax.axis_index("col")
    place = iota((8, GRID), 0)
    own_first = (iota((8, GRID), 1) == row * FIRST + place).astype(BF16)
    own_second = (iota((8, GRID), 1) == col * SECOND + place).astype(BF16)
    ones = jnp.ones((GRID, 128), BF16)
    for k in range(BINS):
        block = table[k, 2]
        block = jnp.concatenate([block, block], axis=1)
        for c in range(2):
            third[c * GRID : (c + 1) * GRID, k * 128 : (k + 1) * 128] = block
        rows = jnp.dot(own_first, table[k, 0], preferred_element_type=F32)
        for i in range(FIRST):
            first[i * BINS + k : i * BINS + k + 1, :] = rows[i : i + 1]
        rows = jnp.dot(own_second, table[k, 1], preferred_element_type=F32).astype(BF16)
        second_sums[k] = jnp.dot(rows, ones, preferred_element_type=F32)
    shape = (GRID, 128)
    wave_first = iota(shape, 0) - CENTRE
    wave_third = iota(shape, 1) % GRID - CENTRE
    quadrant = jnp.where(wave_first * wave_third >= 0, 0, 1)
    own = quadrant == iota(shape, 1) // GRID
    height = jnp.where(own, 16 * jnp.abs(wave_third), 16 * GRID * GRID)
    width = jnp.abs(wave_first)
    rows = first[...].astype(BF16)
    for k in range(SLOPES):
        held = jnp.where(height <= (k + SLOPE_MIN) * width, 1.0, 0.0).astype(BF16)
        grown[:, k * 128 : (k + 1) * 128] = jnp.dot(rows, held, preferred_element_type=F32)


def operators(table):
    return pl.pallas_call(
        operators_kernel,
        out_shape=(
            jax.ShapeDtypeStruct((128, BINS * 128), BF16),
            jax.ShapeDtypeStruct((FIRST * BINS, SLOPES * 128), F32),
            jax.ShapeDtypeStruct((BINS, SECOND, 128), F32),
        ),
        in_specs=[VMEM],
        out_specs=(VMEM,) * 3,
        scratch_shapes=[pltpu.VMEM((FIRST * BINS, GRID), F32)],
        compiler_params=SMALL,
        cost_estimate=pl.CostEstimate(flops=10**8, bytes_accessed=2**20, transcendentals=0),
        name="operators",
    )(table)


def divide_kernel(parts, third, grown, second_sums, out, left):
    total = parts[0]
    for k in range(1, COLS):
        total = total + parts[k]
    counts = total[OWN : OWN + 8]
    low = iota((8, 128), 1) < GRID
    held = [[jnp.zeros((8, 128), F32) for _ in range(2)] for _ in range(FIRST)]
    for k in range(SLOPES):
        for upper in range(2):
            lane = upper * 64 + k
            spread = jnp.where(
                low,
                jnp.broadcast_to(counts[:, lane : lane + 1], (8, 128)),
                jnp.broadcast_to(counts[:, lane + 32 : lane + 33], (8, 128)),
            )
            for i in range(FIRST):
                start = i * BINS + upper * 8
                held[i][upper] += spread * grown[start : start + 8, k * 128 : k * 128 + 128]
    for k in range(BINS):
        sums = second_sums[k]
        for i in range(FIRST):
            value = sums * held[i][k // 8][k % 8 : k % 8 + 1, :]
            upper = value.astype(BF16)
            lower = (value - upper.astype(F32)).astype(BF16)
            lanes = slice(k * 128, k * 128 + 128)
            left[i * SECOND : (i + 1) * SECOND, lanes] = upper.astype(F32)
            left[OWN + i * SECOND : OWN + (i + 1) * SECOND, lanes] = lower.astype(F32)
    weight = lax.dot_general(
        left[...].astype(BF16), third[...], (((1,), (1,)), ((), ())), preferred_element_type=F32
    )
    out[...] = total[0:OWN] / (weight[0:OWN] + weight[OWN:] + 1.0)


def divide(parts, third, grown, second_sums):
    return pl.pallas_call(
        divide_kernel,
        out_shape=jax.ShapeDtypeStruct((OWN, 128), F32),
        in_specs=[VMEM] * 4,
        out_specs=VMEM,
        scratch_shapes=[pltpu.VMEM((2 * OWN, BINS * 128), F32)],
        compiler_params=SMALL,
        name="divide",
    )(parts, third, grown, second_sums)


def spectra_kernel(own, other, out, maps, rows):
    on_first = lax.axis_index("half") == 0
    a, b = own[...], other[...]
    cross = a * b
    own_power, other_power = a * a, b * b
    power_first = jnp.where(on_first, own_power, other_power)
    power_second = jnp.where(on_first, other_power, own_power)
    index = iota((OWN, 128), 0)
    first = index // SECOND + lax.axis_index(ROW) * FIRST - CENTRE
    second = index % SECOND + lax.axis_index("col") * SECOND - CENTRE
    third = iota((OWN, 128), 1) % GRID - CENTRE
    radius_sq = first * first + second * second + third * third
    rows[...] = jnp.zeros_like(rows)
    for k in range(SHELLS):
        least = 0 if k == 0 else (k + 3) ** 2
        inside = (radius_sq >= least) & (radius_sq < (k + 4) ** 2)
        for j, value in enumerate((cross, power_first, power_second)):
            rows[j * 32 + k : j * 32 + k + 1, :] = jnp.sum(
                jnp.where(inside, value, 0.0), axis=0, keepdims=True
            )
    rest = rows[...]
    ones = jnp.ones((8, 128), BF16)
    total = jnp.zeros((8, 128), F32)
    for _ in range(3):
        piece = rest.astype(BF16)
        rest = rest - piece.astype(F32)
        total += lax.dot_general(ones, piece, (((1,), (1,)), ((), ())), preferred_element_type=F32)
    for k in range(ROWS):
        out[k] = total
    low = iota((SECOND // 2, 128), 1) < GRID
    for i in range(FIRST):
        even = own[pl.ds(i * SECOND, SECOND // 2, stride=2), :]
        odd = own[pl.ds(i * SECOND + 1, SECOND // 2, stride=2), :]
        real = jnp.where(low, even, pltpu.roll(odd, 64, 1))
        imag = jnp.where(low, pltpu.roll(even, 64, 1), odd)
        for j in range(SECOND // 2):
            lanes = slice(j * 128, j * 128 + 128)
            maps[0, 0, i : i + 1, lanes] = real[j : j + 1]
            maps[0, 1, i : i + 1, lanes] = imag[j : j + 1]


def spectra(own, other):
    return pl.pallas_call(
        spectra_kernel,
        out_shape=(
            jax.ShapeDtypeStruct((ROWS, 8, 128), F32),
            jax.ShapeDtypeStruct((1, 2, FIRST, SECOND * GRID), F32),
        ),
        in_specs=[VMEM, VMEM],
        out_specs=(VMEM, VMEM),
        scratch_shapes=[pltpu.VMEM((128, 128), F32)],
        compiler_params=SMALL,
        name="spectra",
    )(own, other)


def spread_kernel(parts, out):
    total = jnp.sum(parts[...], axis=0)
    for k in range(COLS):
        out[k] = total


def spread_sum(parts):
    return pl.pallas_call(
        spread_kernel,
        out_shape=jax.ShapeDtypeStruct((COLS, 8, 128), F32),
        in_specs=[VMEM],
        out_specs=VMEM,
        compiler_params=SMALL,
        name="spread_sum",
    )(parts)


def finish_kernel(parts, counts, power, correlation):
    total = jnp.sum(parts[...], axis=0)
    cross = total[0:1, 0:SHELLS]
    first = total[0:1, 32 : 32 + SHELLS]
    second = total[0:1, 64 : 64 + SHELLS]
    power[0:1, :] = first / counts[...]
    power[1:2, :] = second / counts[...]
    correlation[...] = cross / jnp.sqrt(first * second + 1e-06)


def finish(parts, counts):
    return pl.pallas_call(
        finish_kernel,
        out_shape=(
            jax.ShapeDtypeStruct((2, SHELLS), F32),
            jax.ShapeDtypeStruct((1, SHELLS), F32),
        ),
        in_specs=[VMEM, VMEM],
        out_specs=(VMEM, VMEM),
        compiler_params=SMALL,
        name="finish",
    )(parts, counts)


def shifted(shift, swapped=False):
    pairs = []
    for half in range(2):
        for x in range(SIDE):
            for y in range(SIDE):
                along_x = (half == 0) != swapped
                to_x = (x + shift) % SIDE if along_x else x
                to_y = y if along_x else (y + shift) % SIDE
                pairs.append((half * ROWS + x * SIDE + y, half * ROWS + to_x * SIDE + to_y))
    return pairs


def shell_counts():
    wave = np.arange(GRID) - CENTRE
    radius_sq = (wave[:, None, None] ** 2 + wave[None, :, None] ** 2 + wave[None, None, :] ** 2).reshape(-1)
    bounds = np.arange(4, CENTRE) ** 2
    shell = np.searchsorted(bounds, radius_sq, side="right")
    inside = radius_sq < CENTRE * CENTRE
    return np.bincount(shell[inside], minlength=SHELLS).astype(np.float32)[None]


def local(particles, orient_bin, tilt_slope, table):
    inputs = [
        pltpu.with_memory_space_constraint(x, pltpu.HBM)
        for x in (particles, orient_bin, tilt_slope, table)
    ]
    *held, far_low, far_high = first_slab(*inputs)
    far_low = lax.ppermute(far_low, HALF_ROW, shifted(1))
    far_high = lax.ppermute(far_high, HALF_ROW, shifted(3))
    after_high, before_low = direct_slabs(*held)
    after_high = lax.ppermute(after_high, HALF_ROW, shifted(1))
    before_low = lax.ppermute(before_low, HALF_ROW, shifted(3))
    after_low, before_high, own = other_slabs(*held)
    after_low, before_high = add_far(after_low, far_low, before_high, far_high)
    after_low = lax.ppermute(after_low, HALF_ROW, shifted(1))
    before_high = lax.ppermute(before_high, HALF_ROW, shifted(3))
    prepared = operators(table)
    parts = [own, after_low, after_high, before_low, before_high]
    *others, own = gather(*parts)
    parts = [
        lax.ppermute(block, HALF_ROW, shifted(shift, True))
        for shift, block in zip((2, 1, 3), others, strict=True)
    ]
    blocks = reduce(own, *parts)
    parts = lax.all_to_all(blocks, "col", 0, 0, tiled=True)
    own = divide(parts, *prepared)
    other = lax.ppermute(own, "half", [(0, 1), (1, 0)])
    sums, half_maps = spectra(own, other)
    parts = lax.all_to_all(sums, ROW, 0, 0, tiled=True)
    parts = lax.all_to_all(spread_sum(parts), "col", 0, 0, tiled=True)
    power, correlation = finish(parts, jnp.asarray(shell_counts()))
    return half_maps, power, correlation


def solution(mesh):
    torus = Mesh(
        mesh.devices.reshape(mesh.shape["half"], 4, 4, mesh.shape["col"]),
        ("half", "row_0", "row_1", "col"),
    )
    in_specs = (P(HALF_ROW_COL, None, None, None), P(HALF_ROW_COL), P(HALF_ROW_COL, None), P())
    out_specs = (P("half", None, ROW, "col"), P(), P("half", None))
    return jax.shard_map(local, mesh=torus, in_specs=in_specs, out_specs=out_specs, check_vma=False)
```

```python
import jax
import jax.numpy as jnp
import numpy as np
from jax import lax
from jax.experimental import pallas as pl
from jax.experimental.pallas import tpu as pltpu
from jax.sharding import Mesh
from jax.sharding import PartitionSpec as P

SHELLS = 29
GRID = 64
CENTRE = GRID // 2
BINS = 16
ROWS = 16
COLS = 8
FIRST = GRID // ROWS
SECOND = GRID // COLS
SLOPE_MIN = 12
SLOPES = 29
SIDE = 4
PITCH = 68
BLOCK = FIRST * GRID
OWN = FIRST * SECOND
ROW = ("row_0", "row_1")
HALF_ROW = ("half", "row_0", "row_1")
HALF_ROW_COL = ("half", "row_0", "row_1", "col")
F32 = jnp.float32
BF16 = jnp.bfloat16
VMEM = pl.BlockSpec(memory_space=pltpu.VMEM)
HBM = pl.BlockSpec(memory_space=pltpu.HBM)
SMALL = pltpu.CompilerParams(vmem_limit_bytes=6 * 2**20)


def iota(shape, dim):
    return lax.broadcasted_iota(jnp.int32, shape, dim)


def wedge_tile(slope_first, slope_second):
    wave_first = iota((GRID, 128), 0) - CENTRE
    wave_third = iota((GRID, 128), 1) % GRID - CENTRE
    limit = jnp.where(wave_first * wave_third >= 0, slope_first, slope_second)
    inside = 16 * jnp.abs(wave_third) <= limit * jnp.abs(wave_first)
    return jnp.where(inside, 1.0, 0.0).astype(BF16)


def histogram_tile(bins, slopes):
    row, lane = iota((8, 128), 0), iota((8, 128), 1)
    total = jnp.zeros((8, 128), F32)
    for p in range(2):
        for quadrant in range(2):
            place = (bins[p] // 8) * 64 + quadrant * 32 + slopes[p, quadrant] - SLOPE_MIN
            total += jnp.where((row == bins[p] % 8) & (lane == place), 1.0, 0.0)
    return total


def compute_slab(shift, inners, planes, second, third, out, counts=None):
    on_first = lax.axis_index("half") == 0
    mine = jnp.where(on_first, lax.axis_index("row_0"), lax.axis_index("row_1"))
    outer = lax.rem(mine + shift, SIDE)
    for n, inner in enumerate(inners):
        row = jnp.where(on_first, outer * SIDE + inner, inner * SIDE + outer)
        for i in range(FIRST):
            parts = []
            for p in range(2):
                plane = planes[p, pl.ds(row * FIRST + i, GRID, stride=PITCH), :].astype(BF16)
                along = jnp.dot(second[p], plane, preferred_element_type=F32)
                parts.append(along.astype(BF16))
            full = jnp.dot(jnp.concatenate(parts, axis=1), third[...], preferred_element_type=F32)
            for q in range(COLS):
                start = n * BLOCK + (q * FIRST + i) * SECOND
                out[start : start + SECOND, :] = full[q * SECOND : (q + 1) * SECOND]
    if counts is not None:
        out[len(inners) * BLOCK : len(inners) * BLOCK + 8, :] = counts[...]


LOW = (0, 1)
HIGH = (2, 3)
HALF_SLAB = jax.ShapeDtypeStruct((2 * BLOCK, 128), F32)
HALF_SLAB_COUNTS = jax.ShapeDtypeStruct((2 * BLOCK + 8, 128), F32)
SLAB = jax.ShapeDtypeStruct((SIDE * BLOCK + 8, 128), F32)


def first_kernel(bins_in, slopes_in, particles, table, planes, second, third, counts, far_low, far_high, volume, chosen, bins, slopes, sem):
    scalars = [
        pltpu.make_async_copy(bins_in, bins, sem.at[6]),
        pltpu.make_async_copy(slopes_in, slopes, sem.at[7]),
    ]
    volumes = [
        pltpu.make_async_copy(
            particles.at[:, :, :, pl.ds(k * 1024, 1024)],
            volume.at[:, :, :, pl.ds(k * 1024, 1024)],
            sem.at[k],
        )
        for k in range(4)
    ]
    for copy in (*scalars, volumes[0]):
        copy.start()
    third[...] = jnp.zeros_like(third)
    low = iota((GRID, 128), 1) < GRID
    for copy in scalars:
        copy.wait()
    tables = [
        pltpu.make_async_copy(table.at[bins[p]], chosen.at[p], sem.at[4 + p]) for p in range(2)
    ]
    for copy in (*tables, *volumes[1:]):
        copy.start()
    wedges = [
        jnp.concatenate([wedge_tile(slopes[p, 0], slopes[p, 1])] * 4, axis=1) for p in range(2)
    ]
    counts[...] = histogram_tile(bins, slopes)
    for copy in tables:
        copy.wait()
    for p in range(2):
        second[p] = chosen[p, 1]
        transposed = chosen[p, 2].astype(F32).T.astype(BF16)
        for c in range(2):
            third[p * 128 + c * 64 : p * 128 + c * 64 + 64, c * 64 : c * 64 + 64] = transposed
    first = [chosen[p, 0] for p in range(2)]

    def transform(chunk):
        for p in range(2):
            tiles = []
            for j in range(2):
                tile = pl.ds(pl.multiple_of(chunk * 256 + j * 128, 128), 128)
                real, imag = (volume[p, c, :, tile] for c in range(2))
                tiles.append(jnp.concatenate([real[:, :GRID], imag[:, :GRID]], axis=1))
                tiles.append(jnp.concatenate([real[:, GRID:], imag[:, GRID:]], axis=1))
            both = jnp.concatenate(tiles, axis=1)
            along = jnp.dot(first[p], both * wedges[p], preferred_element_type=F32)
            for j in range(4):
                base = pl.multiple_of((chunk * 4 + j) * PITCH, 4)
                planes[p, pl.ds(base, GRID), :] = along[:, j * 128 : j * 128 + 128]

    for k in range(4):
        volumes[k].wait()

        @pl.loop(k * 4, k * 4 + 4, unroll=4)
        def _(chunk):
            transform(chunk)

    compute_slab(2, LOW, planes, second, third, far_low, counts)
    compute_slab(2, HIGH, planes, second, third, far_high)


def first_slab(particles, orient_bin, tilt_slope, table):
    return pl.pallas_call(
        first_kernel,
        out_shape=(
            jax.ShapeDtypeStruct((2, GRID * PITCH, 128), F32),
            jax.ShapeDtypeStruct((2, GRID, GRID), BF16),
            jax.ShapeDtypeStruct((256, 128), BF16),
            jax.ShapeDtypeStruct((8, 128), F32),
            HALF_SLAB_COUNTS,
            HALF_SLAB,
        ),
        in_specs=[HBM] * 4,
        out_specs=(VMEM,) * 6,
        scratch_shapes=[
            pltpu.VMEM((2, 2, GRID, GRID * GRID), BF16),
            pltpu.VMEM((2, 3, GRID, GRID), BF16),
            pltpu.SMEM((2,), jnp.int32),
            pltpu.SMEM((2, 2), jnp.int32),
            pltpu.SemaphoreType.DMA((8,)),
        ],
        compiler_params=pltpu.CompilerParams(vmem_limit_bytes=20 * 2**20),
        cost_estimate=pl.CostEstimate(flops=10**9, bytes_accessed=4 * 2**20, transcendentals=0),
        name="first_slab",
    )(orient_bin, tilt_slope, particles, table)


def direct_kernel(planes, second, third, counts, after_high, before_low):
    compute_slab(1, HIGH, planes, second, third, after_high)
    compute_slab(3, LOW, planes, second, third, before_low, counts)


def direct_slabs(planes, second, third, counts):
    return pl.pallas_call(
        direct_kernel,
        out_shape=(HALF_SLAB, HALF_SLAB_COUNTS),
        in_specs=[VMEM] * 4,
        out_specs=(VMEM,) * 2,
        compiler_params=SMALL,
        cost_estimate=pl.CostEstimate(flops=10**9, bytes_accessed=2**20, transcendentals=0),
        name="direct_slabs",
    )(planes, second, third, counts)


def other_kernel(planes, second, third, counts, after_low, before_high, own):
    compute_slab(1, LOW, planes, second, third, after_low, counts)
    compute_slab(3, HIGH, planes, second, third, before_high)
    compute_slab(0, LOW + HIGH, planes, second, third, own, counts)


def other_slabs(planes, second, third, counts):
    return pl.pallas_call(
        other_kernel,
        out_shape=(HALF_SLAB_COUNTS, HALF_SLAB, SLAB),
        in_specs=[VMEM] * 4,
        out_specs=(VMEM,) * 3,
        compiler_params=SMALL,
        cost_estimate=pl.CostEstimate(flops=10**9, bytes_accessed=2**20, transcendentals=0),
        name="other_slabs",
    )(planes, second, third, counts)


def add_kernel(after_low, far_low, before_high, far_high, after_out, before_out):
    after_out[...] = after_low[...] + far_low[...]
    before_out[...] = before_high[...] + far_high[...]


def add_far(after_low, far_low, before_high, far_high):
    return pl.pallas_call(
        add_kernel,
        out_shape=(HALF_SLAB_COUNTS, HALF_SLAB),
        in_specs=[VMEM] * 4,
        out_specs=(VMEM,) * 2,
        compiler_params=SMALL,
        cost_estimate=pl.CostEstimate(flops=10**8, bytes_accessed=2**20, transcendentals=0),
        name="add_far",
    )(after_low, far_low, before_high, far_high)


def gather_kernel(own, after_low, after_high, before_low, before_high, *refs):
    *outs, sums = refs
    on_first = lax.axis_index("half") == 0
    mine = jnp.where(on_first, lax.axis_index("row_1"), lax.axis_index("row_0"))
    half = 2 * BLOCK
    tail = pl.ds(half, 8)
    counts = own[pl.ds(2 * half, 8), :] + after_low[tail, :] + before_low[tail, :]
    for n, parts in enumerate(((after_low, before_low), (after_high, before_high))):
        span = pl.ds(n * half, half)
        sums[span, :] = own[span, :] + parts[0][0:half, :] + parts[1][0:half, :]
    for shift, out in zip((2, 1, 3, 0), outs, strict=True):
        span = pl.ds(pl.multiple_of(lax.rem(mine + shift, SIDE) * BLOCK, 8), BLOCK)
        out[0:BLOCK, :] = sums[span, :]
        out[BLOCK : BLOCK + 8, :] = counts


def gather(*parts):
    return pl.pallas_call(
        gather_kernel,
        out_shape=(jax.ShapeDtypeStruct((BLOCK + 8, 128), F32),) * SIDE,
        in_specs=[VMEM] * len(parts),
        out_specs=(VMEM,) * SIDE,
        scratch_shapes=[pltpu.VMEM((SIDE * BLOCK, 128), F32)],
        compiler_params=SMALL,
        name="gather",
    )(*parts)


def reduce_kernel(*refs):
    *parts, out = refs
    tail = pl.ds(BLOCK, 8)
    counts = parts[0][tail, :]
    for part in parts[1:]:
        counts = counts + part[tail, :]
    for n in range(COLS):
        span = pl.ds(n * OWN, OWN)
        total = parts[0][span, :]
        for part in parts[1:]:
            total = total + part[span, :]
        out[n, 0:OWN, :] = total
        out[n, OWN : OWN + 8, :] = counts


def reduce(*parts):
    return pl.pallas_call(
        reduce_kernel,
        out_shape=jax.ShapeDtypeStruct((COLS, OWN + 8, 128), F32),
        in_specs=[VMEM] * len(parts),
        out_specs=VMEM,
        compiler_params=SMALL,
        name="reduce",
    )(*parts)


def operators_kernel(table, third, grown, second_sums, first):
    row, col = lax.axis_index(ROW), lax.axis_index("col")
    place = iota((8, GRID), 0)
    own_first = (iota((8, GRID), 1) == row * FIRST + place).astype(BF16)
    own_second = (iota((8, GRID), 1) == col * SECOND + place).astype(BF16)
    ones = jnp.ones((GRID, 128), BF16)
    for k in range(BINS):
        block = table[k, 2]
        block = jnp.concatenate([block, block], axis=1)
        for c in range(2):
            third[c * GRID : (c + 1) * GRID, k * 128 : (k + 1) * 128] = block
        rows = jnp.dot(own_first, table[k, 0], preferred_element_type=F32)
        for i in range(FIRST):
            first[i * BINS + k : i * BINS + k + 1, :] = rows[i : i + 1]
        rows = jnp.dot(own_second, table[k, 1], preferred_element_type=F32).astype(BF16)
        second_sums[k] = jnp.dot(rows, ones, preferred_element_type=F32)
    shape = (GRID, 128)
    wave_first = iota(shape, 0) - CENTRE
    wave_third = iota(shape, 1) % GRID - CENTRE
    quadrant = jnp.where(wave_first * wave_third >= 0, 0, 1)
    own = quadrant == iota(shape, 1) // GRID
    height = jnp.where(own, 16 * jnp.abs(wave_third), 16 * GRID * GRID)
    width = jnp.abs(wave_first)
    rows = first[...].astype(BF16)
    for k in range(SLOPES):
        held = jnp.where(height <= (k + SLOPE_MIN) * width, 1.0, 0.0).astype(BF16)
        grown[:, k * 128 : (k + 1) * 128] = jnp.dot(rows, held, preferred_element_type=F32)


def operators(table):
    return pl.pallas_call(
        operators_kernel,
        out_shape=(
            jax.ShapeDtypeStruct((128, BINS * 128), BF16),
            jax.ShapeDtypeStruct((FIRST * BINS, SLOPES * 128), F32),
            jax.ShapeDtypeStruct((BINS, SECOND, 128), F32),
        ),
        in_specs=[VMEM],
        out_specs=(VMEM,) * 3,
        scratch_shapes=[pltpu.VMEM((FIRST * BINS, GRID), F32)],
        compiler_params=SMALL,
        cost_estimate=pl.CostEstimate(flops=10**8, bytes_accessed=2**20, transcendentals=0),
        name="operators",
    )(table)


def divide_kernel(parts, third, grown, second_sums, out, left):
    total = parts[0]
    for k in range(1, COLS):
        total = total + parts[k]
    counts = total[OWN : OWN + 8]
    low = iota((8, 128), 1) < GRID
    held = [[jnp.zeros((8, 128), F32) for _ in range(2)] for _ in range(FIRST)]
    for k in range(SLOPES):
        for upper in range(2):
            lane = upper * 64 + k
            spread = jnp.where(
                low,
                jnp.broadcast_to(counts[:, lane : lane + 1], (8, 128)),
                jnp.broadcast_to(counts[:, lane + 32 : lane + 33], (8, 128)),
            )
            for i in range(FIRST):
                start = i * BINS + upper * 8
                held[i][upper] += spread * grown[start : start + 8, k * 128 : k * 128 + 128]
    for k in range(BINS):
        sums = second_sums[k]
        for i in range(FIRST):
            value = sums * held[i][k // 8][k % 8 : k % 8 + 1, :]
            upper = value.astype(BF16)
            lower = (value - upper.astype(F32)).astype(BF16)
            lanes = slice(k * 128, k * 128 + 128)
            left[i * SECOND : (i + 1) * SECOND, lanes] = upper.astype(F32)
            left[OWN + i * SECOND : OWN + (i + 1) * SECOND, lanes] = lower.astype(F32)
    weight = lax.dot_general(
        left[...].astype(BF16), third[...], (((1,), (1,)), ((), ())), preferred_element_type=F32
    )
    out[...] = total[0:OWN] / (weight[0:OWN] + weight[OWN:] + 1.0)


def divide(parts, third, grown, second_sums):
    return pl.pallas_call(
        divide_kernel,
        out_shape=jax.ShapeDtypeStruct((OWN, 128), F32),
        in_specs=[VMEM] * 4,
        out_specs=VMEM,
        scratch_shapes=[pltpu.VMEM((2 * OWN, BINS * 128), F32)],
        compiler_params=SMALL,
        name="divide",
    )(parts, third, grown, second_sums)


def spectra_kernel(own, other, out, rows):
    on_first = lax.axis_index("half") == 0
    a, b = own[...], other[...]
    cross = a * b
    own_power, other_power = a * a, b * b
    power_first = jnp.where(on_first, own_power, other_power)
    power_second = jnp.where(on_first, other_power, own_power)
    index = iota((OWN, 128), 0)
    first = index // SECOND + lax.axis_index(ROW) * FIRST - CENTRE
    second = index % SECOND + lax.axis_index("col") * SECOND - CENTRE
    third = iota((OWN, 128), 1) % GRID - CENTRE
    radius_sq = first * first + second * second + third * third
    rows[...] = jnp.zeros_like(rows)
    for k in range(SHELLS):
        least = 0 if k == 0 else (k + 3) ** 2
        inside = (radius_sq >= least) & (radius_sq < (k + 4) ** 2)
        for j, value in enumerate((cross, power_first, power_second)):
            rows[j * 32 + k : j * 32 + k + 1, :] = jnp.sum(
                jnp.where(inside, value, 0.0), axis=0, keepdims=True
            )
    rest = rows[...]
    ones = jnp.ones((8, 128), BF16)
    total = jnp.zeros((8, 128), F32)
    for _ in range(3):
        piece = rest.astype(BF16)
        rest = rest - piece.astype(F32)
        total += lax.dot_general(ones, piece, (((1,), (1,)), ((), ())), preferred_element_type=F32)
    for k in range(ROWS):
        out[k] = total[0:1]


def spectra(own, other):
    return pl.pallas_call(
        spectra_kernel,
        out_shape=jax.ShapeDtypeStruct((ROWS, 1, 128), F32),
        in_specs=[VMEM, VMEM],
        out_specs=VMEM,
        scratch_shapes=[pltpu.VMEM((128, 128), F32)],
        compiler_params=SMALL,
        name="spectra",
    )(own, other)


def spread_kernel(parts, out):
    total = jnp.sum(parts[...], axis=0)
    for k in range(COLS):
        out[k] = total


def spread_sum(parts):
    return pl.pallas_call(
        spread_kernel,
        out_shape=jax.ShapeDtypeStruct((COLS, 1, 128), F32),
        in_specs=[VMEM],
        out_specs=VMEM,
        compiler_params=SMALL,
        name="spread_sum",
    )(parts)


def finish_kernel(parts, own, counts, maps, power, correlation):
    total = jnp.sum(parts[...], axis=0)
    cross = total[0:1, 0:SHELLS]
    first = total[0:1, 32 : 32 + SHELLS]
    second = total[0:1, 64 : 64 + SHELLS]
    power[0:1, :] = first / counts[...]
    power[1:2, :] = second / counts[...]
    correlation[...] = cross / jnp.sqrt(first * second + 1e-06)
    low = iota((SECOND // 2, 128), 1) < GRID
    for i in range(FIRST):
        even = own[pl.ds(i * SECOND, SECOND // 2, stride=2), :]
        odd = own[pl.ds(i * SECOND + 1, SECOND // 2, stride=2), :]
        real = jnp.where(low, even, pltpu.roll(odd, 64, 1))
        imag = jnp.where(low, pltpu.roll(even, 64, 1), odd)
        for j in range(SECOND // 2):
            lanes = slice(j * 128, j * 128 + 128)
            maps[0, 0, i : i + 1, lanes] = real[j : j + 1]
            maps[0, 1, i : i + 1, lanes] = imag[j : j + 1]


def finish(parts, own, counts):
    return pl.pallas_call(
        finish_kernel,
        out_shape=(
            jax.ShapeDtypeStruct((1, 2, FIRST, SECOND * GRID), F32),
            jax.ShapeDtypeStruct((2, SHELLS), F32),
            jax.ShapeDtypeStruct((1, SHELLS), F32),
        ),
        in_specs=[VMEM] * 3,
        out_specs=(VMEM,) * 3,
        compiler_params=SMALL,
        name="finish",
    )(parts, own, counts)


def shifted(shift, swapped=False):
    pairs = []
    for half in range(2):
        for x in range(SIDE):
            for y in range(SIDE):
                along_x = (half == 0) != swapped
                to_x = (x + shift) % SIDE if along_x else x
                to_y = y if along_x else (y + shift) % SIDE
                pairs.append((half * ROWS + x * SIDE + y, half * ROWS + to_x * SIDE + to_y))
    return pairs


def shell_counts():
    wave = np.arange(GRID) - CENTRE
    radius_sq = (wave[:, None, None] ** 2 + wave[None, :, None] ** 2 + wave[None, None, :] ** 2).reshape(-1)
    bounds = np.arange(4, CENTRE) ** 2
    shell = np.searchsorted(bounds, radius_sq, side="right")
    inside = radius_sq < CENTRE * CENTRE
    return np.bincount(shell[inside], minlength=SHELLS).astype(np.float32)[None]


def local(particles, orient_bin, tilt_slope, table):
    inputs = [
        pltpu.with_memory_space_constraint(x, pltpu.HBM)
        for x in (particles, orient_bin, tilt_slope, table)
    ]
    *held, far_low, far_high = first_slab(*inputs)
    far_low = lax.ppermute(far_low, HALF_ROW, shifted(1))
    far_high = lax.ppermute(far_high, HALF_ROW, shifted(3))
    after_high, before_low = direct_slabs(*held)
    after_high = lax.ppermute(after_high, HALF_ROW, shifted(1))
    before_low = lax.ppermute(before_low, HALF_ROW, shifted(3))
    after_low, before_high, own = other_slabs(*held)
    after_low, before_high = add_far(after_low, far_low, before_high, far_high)
    after_low = lax.ppermute(after_low, HALF_ROW, shifted(1))
    before_high = lax.ppermute(before_high, HALF_ROW, shifted(3))
    prepared = operators(table)
    parts = [own, after_low, after_high, before_low, before_high]
    *others, own = gather(*parts)
    parts = [
        lax.ppermute(block, HALF_ROW, shifted(shift, True))
        for shift, block in zip((2, 1, 3), others, strict=True)
    ]
    blocks = reduce(own, *parts)
    parts = lax.all_to_all(blocks, "col", 0, 0, tiled=True)
    own = divide(parts, *prepared)
    other = lax.ppermute(own, "half", [(0, 1), (1, 0)])
    parts = lax.all_to_all(spectra(own, other), ROW, 0, 0, tiled=True)
    parts = lax.all_to_all(spread_sum(parts), "col", 0, 0, tiled=True)
    half_maps, power, correlation = finish(parts, own, jnp.asarray(shell_counts()))
    return half_maps, power, correlation


def solution(mesh):
    torus = Mesh(
        mesh.devices.reshape(mesh.shape["half"], 4, 4, mesh.shape["col"]),
        ("half", "row_0", "row_1", "col"),
    )
    in_specs = (P(HALF_ROW_COL, None, None, None), P(HALF_ROW_COL), P(HALF_ROW_COL, None), P())
    out_specs = (P("half", None, ROW, "col"), P(), P("half", None))
    return jax.shard_map(local, mesh=torus, in_specs=in_specs, out_specs=out_specs, check_vma=False)
```

```python
import jax
import jax.numpy as jnp
import numpy as np
from jax import lax
from jax.experimental import pallas as pl
from jax.experimental.pallas import tpu as pltpu
from jax.sharding import Mesh
from jax.sharding import PartitionSpec as P

SHELLS = 29
GRID = 64
CENTRE = GRID // 2
BINS = 16
ROWS = 16
COLS = 8
FIRST = GRID // ROWS
SECOND = GRID // COLS
SLOPE_MIN = 12
SLOPES = 29
SIDE = 4
PITCH = 68
BLOCK = FIRST * GRID
OWN = FIRST * SECOND
ROW = ("row_0", "row_1")
HALF_ROW = ("half", "row_0", "row_1")
HALF_ROW_COL = ("half", "row_0", "row_1", "col")
F32 = jnp.float32
BF16 = jnp.bfloat16
VMEM = pl.BlockSpec(memory_space=pltpu.VMEM)
HBM = pl.BlockSpec(memory_space=pltpu.HBM)
SMALL = pltpu.CompilerParams(vmem_limit_bytes=6 * 2**20)


def iota(shape, dim):
    return lax.broadcasted_iota(jnp.int32, shape, dim)


def wedge_tile(slope_first, slope_second):
    wave_first = iota((GRID, 128), 0) - CENTRE
    wave_third = iota((GRID, 128), 1) % GRID - CENTRE
    limit = jnp.where(wave_first * wave_third >= 0, slope_first, slope_second)
    inside = 16 * jnp.abs(wave_third) <= limit * jnp.abs(wave_first)
    return jnp.where(inside, 1.0, 0.0).astype(BF16)


def histogram_tile(bins, slopes):
    row, lane = iota((8, 128), 0), iota((8, 128), 1)
    total = jnp.zeros((8, 128), F32)
    for p in range(2):
        for quadrant in range(2):
            place = (bins[p] // 8) * 64 + quadrant * 32 + slopes[p, quadrant] - SLOPE_MIN
            total += jnp.where((row == bins[p] % 8) & (lane == place), 1.0, 0.0)
    return total


def compute_slab(shift, inners, planes, second, third, out, counts=None):
    on_first = lax.axis_index("half") == 0
    mine = jnp.where(on_first, lax.axis_index("row_0"), lax.axis_index("row_1"))
    outer = lax.rem(mine + shift, SIDE)
    for n, inner in enumerate(inners):
        row = jnp.where(on_first, outer * SIDE + inner, inner * SIDE + outer)
        for i in range(FIRST):
            parts = []
            for p in range(2):
                plane = planes[p, pl.ds(row * FIRST + i, GRID, stride=PITCH), :].astype(BF16)
                along = jnp.dot(second[p], plane, preferred_element_type=F32)
                parts.append(along.astype(BF16))
            full = jnp.dot(jnp.concatenate(parts, axis=1), third[...], preferred_element_type=F32)
            for q in range(COLS):
                start = n * BLOCK + (q * FIRST + i) * SECOND
                out[start : start + SECOND, :] = full[q * SECOND : (q + 1) * SECOND]
    if counts is not None:
        out[len(inners) * BLOCK : len(inners) * BLOCK + 8, :] = counts[...]


LOW = (0, 1)
HIGH = (2, 3)
HALF_SLAB = jax.ShapeDtypeStruct((2 * BLOCK, 128), F32)
HALF_SLAB_COUNTS = jax.ShapeDtypeStruct((2 * BLOCK + 8, 128), F32)
SLAB = jax.ShapeDtypeStruct((SIDE * BLOCK + 8, 128), F32)


def first_kernel(bins_in, slopes_in, particles, table, planes, second, third, counts, far_low, far_high, volume, chosen, bins, slopes, sem):
    scalars = [
        pltpu.make_async_copy(bins_in, bins, sem.at[6]),
        pltpu.make_async_copy(slopes_in, slopes, sem.at[7]),
    ]
    volumes = [
        pltpu.make_async_copy(
            particles.at[:, :, :, pl.ds(k * 1024, 1024)],
            volume.at[:, :, :, pl.ds(k * 1024, 1024)],
            sem.at[k],
        )
        for k in range(4)
    ]
    whole = pltpu.make_async_copy(table, chosen, sem.at[4])
    for copy in (*scalars, whole, *volumes):
        copy.start()
    third[...] = jnp.zeros_like(third)
    low = iota((GRID, 128), 1) < GRID
    for copy in scalars:
        copy.wait()
    wedges = [
        jnp.concatenate([wedge_tile(slopes[p, 0], slopes[p, 1])] * 4, axis=1) for p in range(2)
    ]
    counts[...] = histogram_tile(bins, slopes)
    whole.wait()
    for p in range(2):
        second[p] = chosen[bins[p], 1]
        transposed = chosen[bins[p], 2].astype(F32).T.astype(BF16)
        for c in range(2):
            third[p * 128 + c * 64 : p * 128 + c * 64 + 64, c * 64 : c * 64 + 64] = transposed
    first = [chosen[bins[p], 0] for p in range(2)]

    def transform(chunk):
        for p in range(2):
            tiles = []
            for j in range(2):
                tile = pl.ds(pl.multiple_of(chunk * 256 + j * 128, 128), 128)
                real, imag = (volume[p, c, :, tile] for c in range(2))
                tiles.append(jnp.concatenate([real[:, :GRID], imag[:, :GRID]], axis=1))
                tiles.append(jnp.concatenate([real[:, GRID:], imag[:, GRID:]], axis=1))
            both = jnp.concatenate(tiles, axis=1)
            along = jnp.dot(first[p], both * wedges[p], preferred_element_type=F32)
            for j in range(4):
                base = pl.multiple_of((chunk * 4 + j) * PITCH, 4)
                planes[p, pl.ds(base, GRID), :] = along[:, j * 128 : j * 128 + 128]

    for k in range(4):
        volumes[k].wait()

        @pl.loop(k * 4, k * 4 + 4, unroll=4)
        def _(chunk):
            transform(chunk)

    compute_slab(2, LOW, planes, second, third, far_low, counts)
    compute_slab(2, HIGH, planes, second, third, far_high)


def first_slab(particles, orient_bin, tilt_slope, table):
    return pl.pallas_call(
        first_kernel,
        out_shape=(
            jax.ShapeDtypeStruct((2, GRID * PITCH, 128), F32),
            jax.ShapeDtypeStruct((2, GRID, GRID), BF16),
            jax.ShapeDtypeStruct((256, 128), BF16),
            jax.ShapeDtypeStruct((8, 128), F32),
            HALF_SLAB_COUNTS,
            HALF_SLAB,
        ),
        in_specs=[HBM] * 4,
        out_specs=(VMEM,) * 6,
        scratch_shapes=[
            pltpu.VMEM((2, 2, GRID, GRID * GRID), BF16),
            pltpu.VMEM((BINS, 3, GRID, GRID), BF16),
            pltpu.SMEM((2,), jnp.int32),
            pltpu.SMEM((2, 2), jnp.int32),
            pltpu.SemaphoreType.DMA((8,)),
        ],
        compiler_params=pltpu.CompilerParams(vmem_limit_bytes=20 * 2**20),
        cost_estimate=pl.CostEstimate(flops=10**9, bytes_accessed=4 * 2**20, transcendentals=0),
        name="first_slab",
    )(orient_bin, tilt_slope, particles, table)


def direct_kernel(planes, second, third, counts, after_high, before_low):
    compute_slab(1, HIGH, planes, second, third, after_high)
    compute_slab(3, LOW, planes, second, third, before_low, counts)


def direct_slabs(planes, second, third, counts):
    return pl.pallas_call(
        direct_kernel,
        out_shape=(HALF_SLAB, HALF_SLAB_COUNTS),
        in_specs=[VMEM] * 4,
        out_specs=(VMEM,) * 2,
        compiler_params=SMALL,
        cost_estimate=pl.CostEstimate(flops=10**9, bytes_accessed=2**20, transcendentals=0),
        name="direct_slabs",
    )(planes, second, third, counts)


def other_kernel(planes, second, third, counts, after_low, before_high, own):
    compute_slab(1, LOW, planes, second, third, after_low, counts)
    compute_slab(3, HIGH, planes, second, third, before_high)
    compute_slab(0, LOW + HIGH, planes, second, third, own, counts)


def other_slabs(planes, second, third, counts):
    return pl.pallas_call(
        other_kernel,
        out_shape=(HALF_SLAB_COUNTS, HALF_SLAB, SLAB),
        in_specs=[VMEM] * 4,
        out_specs=(VMEM,) * 3,
        compiler_params=SMALL,
        cost_estimate=pl.CostEstimate(flops=10**9, bytes_accessed=2**20, transcendentals=0),
        name="other_slabs",
    )(planes, second, third, counts)


def add_kernel(after_low, far_low, before_high, far_high, after_out, before_out):
    after_out[...] = after_low[...] + far_low[...]
    before_out[...] = before_high[...] + far_high[...]


def add_far(after_low, far_low, before_high, far_high):
    return pl.pallas_call(
        add_kernel,
        out_shape=(HALF_SLAB_COUNTS, HALF_SLAB),
        in_specs=[VMEM] * 4,
        out_specs=(VMEM,) * 2,
        compiler_params=SMALL,
        cost_estimate=pl.CostEstimate(flops=10**8, bytes_accessed=2**20, transcendentals=0),
        name="add_far",
    )(after_low, far_low, before_high, far_high)


def gather_kernel(own, after_low, after_high, before_low, before_high, *refs):
    *outs, sums = refs
    on_first = lax.axis_index("half") == 0
    mine = jnp.where(on_first, lax.axis_index("row_1"), lax.axis_index("row_0"))
    half = 2 * BLOCK
    tail = pl.ds(half, 8)
    counts = own[pl.ds(2 * half, 8), :] + after_low[tail, :] + before_low[tail, :]
    for n, parts in enumerate(((after_low, before_low), (after_high, before_high))):
        span = pl.ds(n * half, half)
        sums[span, :] = own[span, :] + parts[0][0:half, :] + parts[1][0:half, :]
    for shift, out in zip((1, 3, 2, 0), outs, strict=True):
        span = pl.ds(pl.multiple_of(lax.rem(mine + shift, SIDE) * BLOCK, 8), BLOCK)
        out[0:BLOCK, :] = sums[span, :]
        out[BLOCK : BLOCK + 8, :] = counts


def gather(*parts):
    return pl.pallas_call(
        gather_kernel,
        out_shape=(jax.ShapeDtypeStruct((BLOCK + 8, 128), F32),) * SIDE,
        in_specs=[VMEM] * len(parts),
        out_specs=(VMEM,) * SIDE,
        scratch_shapes=[pltpu.VMEM((SIDE * BLOCK, 128), F32)],
        compiler_params=SMALL,
        name="gather",
    )(*parts)


def reduce_kernel(*refs):
    *parts, out = refs
    tail = pl.ds(BLOCK, 8)
    counts = parts[0][tail, :]
    for part in parts[1:]:
        counts = counts + part[tail, :]
    for n in range(COLS):
        span = pl.ds(n * OWN, OWN)
        total = parts[0][span, :]
        for part in parts[1:]:
            total = total + part[span, :]
        out[n, 0:OWN, :] = total
        out[n, OWN : OWN + 8, :] = counts


def reduce(*parts):
    return pl.pallas_call(
        reduce_kernel,
        out_shape=jax.ShapeDtypeStruct((COLS, OWN + 8, 128), F32),
        in_specs=[VMEM] * len(parts),
        out_specs=VMEM,
        compiler_params=SMALL,
        name="reduce",
    )(*parts)


def operators_kernel(table, third, grown, second_sums, first):
    row, col = lax.axis_index(ROW), lax.axis_index("col")
    place = iota((8, GRID), 0)
    own_first = (iota((8, GRID), 1) == row * FIRST + place).astype(BF16)
    own_second = (iota((8, GRID), 1) == col * SECOND + place).astype(BF16)
    ones = jnp.ones((GRID, 128), BF16)
    for k in range(BINS):
        block = table[k, 2]
        block = jnp.concatenate([block, block], axis=1)
        for c in range(2):
            third[c * GRID : (c + 1) * GRID, k * 128 : (k + 1) * 128] = block
        rows = jnp.dot(own_first, table[k, 0], preferred_element_type=F32)
        for i in range(FIRST):
            first[i * BINS + k : i * BINS + k + 1, :] = rows[i : i + 1]
        rows = jnp.dot(own_second, table[k, 1], preferred_element_type=F32).astype(BF16)
        second_sums[k] = jnp.dot(rows, ones, preferred_element_type=F32)
    shape = (GRID, 128)
    wave_first = iota(shape, 0) - CENTRE
    wave_third = iota(shape, 1) % GRID - CENTRE
    quadrant = jnp.where(wave_first * wave_third >= 0, 0, 1)
    own = quadrant == iota(shape, 1) // GRID
    height = jnp.where(own, 16 * jnp.abs(wave_third), 16 * GRID * GRID)
    width = jnp.abs(wave_first)
    rows = first[...].astype(BF16)
    for k in range(SLOPES):
        held = jnp.where(height <= (k + SLOPE_MIN) * width, 1.0, 0.0).astype(BF16)
        grown[:, k * 128 : (k + 1) * 128] = jnp.dot(rows, held, preferred_element_type=F32)


def operators(table):
    return pl.pallas_call(
        operators_kernel,
        out_shape=(
            jax.ShapeDtypeStruct((128, BINS * 128), BF16),
            jax.ShapeDtypeStruct((FIRST * BINS, SLOPES * 128), F32),
            jax.ShapeDtypeStruct((BINS, SECOND, 128), F32),
        ),
        in_specs=[VMEM],
        out_specs=(VMEM,) * 3,
        scratch_shapes=[pltpu.VMEM((FIRST * BINS, GRID), F32)],
        compiler_params=SMALL,
        cost_estimate=pl.CostEstimate(flops=10**8, bytes_accessed=2**20, transcendentals=0),
        name="operators",
    )(table)


def divide_kernel(parts, third, grown, second_sums, out, left):
    total = parts[0]
    for k in range(1, COLS):
        total = total + parts[k]
    counts = total[OWN : OWN + 8]
    low = iota((8, 128), 1) < GRID
    held = [[jnp.zeros((8, 128), F32) for _ in range(2)] for _ in range(FIRST)]
    for k in range(SLOPES):
        for upper in range(2):
            lane = upper * 64 + k
            spread = jnp.where(
                low,
                jnp.broadcast_to(counts[:, lane : lane + 1], (8, 128)),
                jnp.broadcast_to(counts[:, lane + 32 : lane + 33], (8, 128)),
            )
            for i in range(FIRST):
                start = i * BINS + upper * 8
                held[i][upper] += spread * grown[start : start + 8, k * 128 : k * 128 + 128]
    for k in range(BINS):
        sums = second_sums[k]
        for i in range(FIRST):
            value = sums * held[i][k // 8][k % 8 : k % 8 + 1, :]
            upper = value.astype(BF16)
            lower = (value - upper.astype(F32)).astype(BF16)
            lanes = slice(k * 128, k * 128 + 128)
            left[i * SECOND : (i + 1) * SECOND, lanes] = upper.astype(F32)
            left[OWN + i * SECOND : OWN + (i + 1) * SECOND, lanes] = lower.astype(F32)
    weight = lax.dot_general(
        left[...].astype(BF16), third[...], (((1,), (1,)), ((), ())), preferred_element_type=F32
    )
    out[...] = total[0:OWN] / (weight[0:OWN] + weight[OWN:] + 1.0)


def divide(parts, third, grown, second_sums):
    return pl.pallas_call(
        divide_kernel,
        out_shape=jax.ShapeDtypeStruct((OWN, 128), F32),
        in_specs=[VMEM] * 4,
        out_specs=VMEM,
        scratch_shapes=[pltpu.VMEM((2 * OWN, BINS * 128), F32)],
        compiler_params=SMALL,
        name="divide",
    )(parts, third, grown, second_sums)


def spectra_kernel(own, other, out, rows):
    on_first = lax.axis_index("half") == 0
    a, b = own[...], other[...]
    cross = a * b
    own_power, other_power = a * a, b * b
    power_first = jnp.where(on_first, own_power, other_power)
    power_second = jnp.where(on_first, other_power, own_power)
    index = iota((OWN, 128), 0)
    first = index // SECOND + lax.axis_index(ROW) * FIRST - CENTRE
    second = index % SECOND + lax.axis_index("col") * SECOND - CENTRE
    third = iota((OWN, 128), 1) % GRID - CENTRE
    radius_sq = first * first + second * second + third * third
    rows[...] = jnp.zeros_like(rows)
    for k in range(SHELLS):
        least = 0 if k == 0 else (k + 3) ** 2
        inside = (radius_sq >= least) & (radius_sq < (k + 4) ** 2)
        for j, value in enumerate((cross, power_first, power_second)):
            rows[j * 32 + k : j * 32 + k + 1, :] = jnp.sum(
                jnp.where(inside, value, 0.0), axis=0, keepdims=True
            )
    rest = rows[...]
    ones = jnp.ones((8, 128), BF16)
    total = jnp.zeros((8, 128), F32)
    for _ in range(3):
        piece = rest.astype(BF16)
        rest = rest - piece.astype(F32)
        total += lax.dot_general(ones, piece, (((1,), (1,)), ((), ())), preferred_element_type=F32)
    for k in range(ROWS):
        out[k] = total[0:1]


def spectra(own, other):
    return pl.pallas_call(
        spectra_kernel,
        out_shape=jax.ShapeDtypeStruct((ROWS, 1, 128), F32),
        in_specs=[VMEM, VMEM],
        out_specs=VMEM,
        scratch_shapes=[pltpu.VMEM((128, 128), F32)],
        compiler_params=SMALL,
        name="spectra",
    )(own, other)


def spread_kernel(parts, out):
    total = jnp.sum(parts[...], axis=0)
    for k in range(COLS):
        out[k] = total


def spread_sum(parts):
    return pl.pallas_call(
        spread_kernel,
        out_shape=jax.ShapeDtypeStruct((COLS, 1, 128), F32),
        in_specs=[VMEM],
        out_specs=VMEM,
        compiler_params=SMALL,
        name="spread_sum",
    )(parts)


def finish_kernel(parts, own, counts, maps, power, correlation):
    total = jnp.sum(parts[...], axis=0)
    cross = total[0:1, 0:SHELLS]
    first = total[0:1, 32 : 32 + SHELLS]
    second = total[0:1, 64 : 64 + SHELLS]
    power[0:1, :] = first / counts[...]
    power[1:2, :] = second / counts[...]
    correlation[...] = cross / jnp.sqrt(first * second + 1e-06)
    low = iota((SECOND // 2, 128), 1) < GRID
    for i in range(FIRST):
        even = own[pl.ds(i * SECOND, SECOND // 2, stride=2), :]
        odd = own[pl.ds(i * SECOND + 1, SECOND // 2, stride=2), :]
        real = jnp.where(low, even, pltpu.roll(odd, 64, 1))
        imag = jnp.where(low, pltpu.roll(even, 64, 1), odd)
        for j in range(SECOND // 2):
            lanes = slice(j * 128, j * 128 + 128)
            maps[0, 0, i : i + 1, lanes] = real[j : j + 1]
            maps[0, 1, i : i + 1, lanes] = imag[j : j + 1]


def finish(parts, own, counts):
    return pl.pallas_call(
        finish_kernel,
        out_shape=(
            jax.ShapeDtypeStruct((1, 2, FIRST, SECOND * GRID), F32),
            jax.ShapeDtypeStruct((2, SHELLS), F32),
            jax.ShapeDtypeStruct((1, SHELLS), F32),
        ),
        in_specs=[VMEM] * 3,
        out_specs=(VMEM,) * 3,
        compiler_params=SMALL,
        name="finish",
    )(parts, own, counts)


def shifted(shift, swapped=False):
    pairs = []
    for half in range(2):
        for x in range(SIDE):
            for y in range(SIDE):
                along_x = (half == 0) != swapped
                to_x = (x + shift) % SIDE if along_x else x
                to_y = y if along_x else (y + shift) % SIDE
                pairs.append((half * ROWS + x * SIDE + y, half * ROWS + to_x * SIDE + to_y))
    return pairs


def shell_counts():
    wave = np.arange(GRID) - CENTRE
    radius_sq = (wave[:, None, None] ** 2 + wave[None, :, None] ** 2 + wave[None, None, :] ** 2).reshape(-1)
    bounds = np.arange(4, CENTRE) ** 2
    shell = np.searchsorted(bounds, radius_sq, side="right")
    inside = radius_sq < CENTRE * CENTRE
    return np.bincount(shell[inside], minlength=SHELLS).astype(np.float32)[None]


def local(particles, orient_bin, tilt_slope, table):
    inputs = [
        pltpu.with_memory_space_constraint(x, pltpu.HBM)
        for x in (particles, orient_bin, tilt_slope, table)
    ]
    *held, far_low, far_high = first_slab(*inputs)
    far_low = lax.ppermute(far_low, HALF_ROW, shifted(1))
    far_high = lax.ppermute(far_high, HALF_ROW, shifted(3))
    after_high, before_low = direct_slabs(*held)
    after_high = lax.ppermute(after_high, HALF_ROW, shifted(1))
    before_low = lax.ppermute(before_low, HALF_ROW, shifted(3))
    after_low, before_high, own = other_slabs(*held)
    after_low, before_high = add_far(after_low, far_low, before_high, far_high)
    after_low = lax.ppermute(after_low, HALF_ROW, shifted(1))
    before_high = lax.ppermute(before_high, HALF_ROW, shifted(3))
    prepared = operators(table)
    parts = [own, after_low, after_high, before_low, before_high]
    *others, own = gather(*parts)
    parts = [
        lax.ppermute(block, HALF_ROW, shifted(shift, True))
        for shift, block in zip((1, 3, 2), others, strict=True)
    ]
    blocks = reduce(own, *parts)
    parts = lax.all_to_all(blocks, "col", 0, 0, tiled=True)
    own = divide(parts, *prepared)
    other = lax.ppermute(own, "half", [(0, 1), (1, 0)])
    parts = lax.all_to_all(spectra(own, other), ROW, 0, 0, tiled=True)
    parts = lax.all_to_all(spread_sum(parts), "col", 0, 0, tiled=True)
    half_maps, power, correlation = finish(parts, own, jnp.asarray(shell_counts()))
    return half_maps, power, correlation


def solution(mesh):
    torus = Mesh(
        mesh.devices.reshape(mesh.shape["half"], 4, 4, mesh.shape["col"]),
        ("half", "row_0", "row_1", "col"),
    )
    in_specs = (P(HALF_ROW_COL, None, None, None), P(HALF_ROW_COL), P(HALF_ROW_COL, None), P())
    out_specs = (P("half", None, ROW, "col"), P(), P("half", None))
    return jax.shard_map(local, mesh=torus, in_specs=in_specs, out_specs=out_specs, check_vma=False)
```

```python
import jax
import jax.numpy as jnp
import numpy as np
from jax import lax
from jax.experimental import pallas as pl
from jax.experimental.pallas import tpu as pltpu
from jax.sharding import Mesh
from jax.sharding import PartitionSpec as P

SHELLS = 29
GRID = 64
CENTRE = GRID // 2
BINS = 16
ROWS = 16
COLS = 8
FIRST = GRID // ROWS
SECOND = GRID // COLS
SLOPE_MIN = 12
SLOPES = 29
SIDE = 4
PITCH = 68
BLOCK = FIRST * GRID
OWN = FIRST * SECOND
ROW = ("row_0", "row_1")
HALF_ROW = ("half", "row_0", "row_1")
HALF_ROW_COL = ("half", "row_0", "row_1", "col")
F32 = jnp.float32
BF16 = jnp.bfloat16
VMEM = pl.BlockSpec(memory_space=pltpu.VMEM)
HBM = pl.BlockSpec(memory_space=pltpu.HBM)
SMALL = pltpu.CompilerParams(vmem_limit_bytes=6 * 2**20)


def iota(shape, dim):
    return lax.broadcasted_iota(jnp.int32, shape, dim)


def wedge_tile(slope_first, slope_second):
    wave_first = iota((GRID, 128), 0) - CENTRE
    wave_third = iota((GRID, 128), 1) % GRID - CENTRE
    limit = jnp.where(wave_first * wave_third >= 0, slope_first, slope_second)
    inside = 16 * jnp.abs(wave_third) <= limit * jnp.abs(wave_first)
    return jnp.where(inside, 1.0, 0.0).astype(BF16)


def histogram_tile(bins, slopes):
    row, lane = iota((8, 128), 0), iota((8, 128), 1)
    total = jnp.zeros((8, 128), F32)
    for p in range(2):
        for quadrant in range(2):
            place = (bins[p] // 8) * 64 + quadrant * 32 + slopes[p, quadrant] - SLOPE_MIN
            total += jnp.where((row == bins[p] % 8) & (lane == place), 1.0, 0.0)
    return total


def compute_slab(shift, inners, planes, second, third, out, counts=None):
    on_first = lax.axis_index("half") == 0
    mine = jnp.where(on_first, lax.axis_index("row_0"), lax.axis_index("row_1"))
    outer = lax.rem(mine + shift, SIDE)
    for n, inner in enumerate(inners):
        row = jnp.where(on_first, outer * SIDE + inner, inner * SIDE + outer)
        for i in range(FIRST):
            parts = []
            for p in range(2):
                plane = planes[p, pl.ds(row * FIRST + i, GRID, stride=PITCH), :].astype(BF16)
                along = jnp.dot(second[p], plane, preferred_element_type=F32)
                parts.append(along.astype(BF16))
            full = jnp.dot(jnp.concatenate(parts, axis=1), third[...], preferred_element_type=F32)
            for q in range(COLS):
                start = n * BLOCK + (q * FIRST + i) * SECOND
                out[start : start + SECOND, :] = full[q * SECOND : (q + 1) * SECOND]
    if counts is not None:
        out[len(inners) * BLOCK : len(inners) * BLOCK + 8, :] = counts[...]


LOW = (0, 1)
HIGH = (2, 3)
HALF_SLAB = jax.ShapeDtypeStruct((2 * BLOCK, 128), F32)
HALF_SLAB_COUNTS = jax.ShapeDtypeStruct((2 * BLOCK + 8, 128), F32)
SLAB = jax.ShapeDtypeStruct((SIDE * BLOCK + 8, 128), F32)


def first_kernel(bins_in, slopes_in, particles, table, planes, second, third, counts, far_low, far_high, volume, chosen, bins, slopes, sem):
    scalars = [
        pltpu.make_async_copy(bins_in, bins, sem.at[6]),
        pltpu.make_async_copy(slopes_in, slopes, sem.at[7]),
    ]
    volumes = [
        pltpu.make_async_copy(
            particles.at[:, :, :, pl.ds(k * 2048, 2048)],
            volume.at[:, :, :, pl.ds(k * 2048, 2048)],
            sem.at[k],
        )
        for k in range(2)
    ]
    whole = pltpu.make_async_copy(table, chosen, sem.at[4])
    for copy in (*scalars, whole, *volumes):
        copy.start()
    third[...] = jnp.zeros_like(third)
    low = iota((GRID, 128), 1) < GRID
    for copy in scalars:
        copy.wait()
    wedges = [
        jnp.concatenate([wedge_tile(slopes[p, 0], slopes[p, 1])] * 4, axis=1) for p in range(2)
    ]
    counts[...] = histogram_tile(bins, slopes)
    whole.wait()
    for p in range(2):
        second[p] = chosen[bins[p], 1]
        transposed = chosen[bins[p], 2].astype(F32).T.astype(BF16)
        for c in range(2):
            third[p * 128 + c * 64 : p * 128 + c * 64 + 64, c * 64 : c * 64 + 64] = transposed
    first = [chosen[bins[p], 0] for p in range(2)]

    def transform(chunk):
        for p in range(2):
            tiles = []
            for j in range(2):
                tile = pl.ds(pl.multiple_of(chunk * 256 + j * 128, 128), 128)
                real, imag = (volume[p, c, :, tile] for c in range(2))
                tiles.append(jnp.concatenate([real[:, :GRID], imag[:, :GRID]], axis=1))
                tiles.append(jnp.concatenate([real[:, GRID:], imag[:, GRID:]], axis=1))
            both = jnp.concatenate(tiles, axis=1)
            along = jnp.dot(first[p], both * wedges[p], preferred_element_type=F32)
            for j in range(4):
                base = pl.multiple_of((chunk * 4 + j) * PITCH, 4)
                planes[p, pl.ds(base, GRID), :] = along[:, j * 128 : j * 128 + 128]

    for k in range(2):
        volumes[k].wait()

        @pl.loop(k * 8, k * 8 + 8, unroll=8)
        def _(chunk):
            transform(chunk)

    compute_slab(2, LOW, planes, second, third, far_low, counts)
    compute_slab(2, HIGH, planes, second, third, far_high)


def first_slab(particles, orient_bin, tilt_slope, table):
    return pl.pallas_call(
        first_kernel,
        out_shape=(
            jax.ShapeDtypeStruct((2, GRID * PITCH, 128), F32),
            jax.ShapeDtypeStruct((2, GRID, GRID), BF16),
            jax.ShapeDtypeStruct((256, 128), BF16),
            jax.ShapeDtypeStruct((8, 128), F32),
            HALF_SLAB_COUNTS,
            HALF_SLAB,
        ),
        in_specs=[HBM] * 4,
        out_specs=(VMEM,) * 6,
        scratch_shapes=[
            pltpu.VMEM((2, 2, GRID, GRID * GRID), BF16),
            pltpu.VMEM((BINS, 3, GRID, GRID), BF16),
            pltpu.SMEM((2,), jnp.int32),
            pltpu.SMEM((2, 2), jnp.int32),
            pltpu.SemaphoreType.DMA((8,)),
        ],
        compiler_params=pltpu.CompilerParams(vmem_limit_bytes=20 * 2**20),
        cost_estimate=pl.CostEstimate(flops=10**9, bytes_accessed=4 * 2**20, transcendentals=0),
        name="first_slab",
    )(orient_bin, tilt_slope, particles, table)


def direct_kernel(planes, second, third, counts, after_high, before_low):
    compute_slab(1, HIGH, planes, second, third, after_high)
    compute_slab(3, LOW, planes, second, third, before_low, counts)


def direct_slabs(planes, second, third, counts):
    return pl.pallas_call(
        direct_kernel,
        out_shape=(HALF_SLAB, HALF_SLAB_COUNTS),
        in_specs=[VMEM] * 4,
        out_specs=(VMEM,) * 2,
        compiler_params=SMALL,
        cost_estimate=pl.CostEstimate(flops=10**9, bytes_accessed=2**20, transcendentals=0),
        name="direct_slabs",
    )(planes, second, third, counts)


def other_kernel(planes, second, third, counts, after_low, before_high, own):
    compute_slab(1, LOW, planes, second, third, after_low, counts)
    compute_slab(3, HIGH, planes, second, third, before_high)
    compute_slab(0, LOW + HIGH, planes, second, third, own, counts)


def other_slabs(planes, second, third, counts):
    return pl.pallas_call(
        other_kernel,
        out_shape=(HALF_SLAB_COUNTS, HALF_SLAB, SLAB),
        in_specs=[VMEM] * 4,
        out_specs=(VMEM,) * 3,
        compiler_params=SMALL,
        cost_estimate=pl.CostEstimate(flops=10**9, bytes_accessed=2**20, transcendentals=0),
        name="other_slabs",
    )(planes, second, third, counts)


def add_kernel(after_low, far_low, before_high, far_high, after_out, before_out):
    after_out[...] = after_low[...] + far_low[...]
    before_out[...] = before_high[...] + far_high[...]


def add_far(after_low, far_low, before_high, far_high):
    return pl.pallas_call(
        add_kernel,
        out_shape=(HALF_SLAB_COUNTS, HALF_SLAB),
        in_specs=[VMEM] * 4,
        out_specs=(VMEM,) * 2,
        compiler_params=SMALL,
        cost_estimate=pl.CostEstimate(flops=10**8, bytes_accessed=2**20, transcendentals=0),
        name="add_far",
    )(after_low, far_low, before_high, far_high)


def gather_kernel(own, after_low, after_high, before_low, before_high, *refs):
    *outs, sums = refs
    on_first = lax.axis_index("half") == 0
    mine = jnp.where(on_first, lax.axis_index("row_1"), lax.axis_index("row_0"))
    half = 2 * BLOCK
    tail = pl.ds(half, 8)
    counts = own[pl.ds(2 * half, 8), :] + after_low[tail, :] + before_low[tail, :]
    for n, parts in enumerate(((after_low, before_low), (after_high, before_high))):
        span = pl.ds(n * half, half)
        sums[span, :] = own[span, :] + parts[0][0:half, :] + parts[1][0:half, :]
    for shift, out in zip((1, 3, 2, 0), outs, strict=True):
        span = pl.ds(pl.multiple_of(lax.rem(mine + shift, SIDE) * BLOCK, 8), BLOCK)
        out[0:BLOCK, :] = sums[span, :]
        out[BLOCK : BLOCK + 8, :] = counts


def gather(*parts):
    return pl.pallas_call(
        gather_kernel,
        out_shape=(jax.ShapeDtypeStruct((BLOCK + 8, 128), F32),) * SIDE,
        in_specs=[VMEM] * len(parts),
        out_specs=(VMEM,) * SIDE,
        scratch_shapes=[pltpu.VMEM((SIDE * BLOCK, 128), F32)],
        compiler_params=SMALL,
        name="gather",
    )(*parts)


def reduce_kernel(*refs):
    *parts, out = refs
    tail = pl.ds(BLOCK, 8)
    counts = parts[0][tail, :]
    for part in parts[1:]:
        counts = counts + part[tail, :]
    for n in range(COLS):
        span = pl.ds(n * OWN, OWN)
        total = parts[0][span, :]
        for part in parts[1:]:
            total = total + part[span, :]
        out[n, 0:OWN, :] = total
        out[n, OWN : OWN + 8, :] = counts


def reduce(*parts):
    return pl.pallas_call(
        reduce_kernel,
        out_shape=jax.ShapeDtypeStruct((COLS, OWN + 8, 128), F32),
        in_specs=[VMEM] * len(parts),
        out_specs=VMEM,
        compiler_params=SMALL,
        name="reduce",
    )(*parts)


def operators_kernel(table, third, grown, second_sums, first):
    row, col = lax.axis_index(ROW), lax.axis_index("col")
    place = iota((8, GRID), 0)
    own_first = (iota((8, GRID), 1) == row * FIRST + place).astype(BF16)
    own_second = (iota((8, GRID), 1) == col * SECOND + place).astype(BF16)
    ones = jnp.ones((GRID, 128), BF16)
    for k in range(BINS):
        block = table[k, 2]
        block = jnp.concatenate([block, block], axis=1)
        for c in range(2):
            third[c * GRID : (c + 1) * GRID, k * 128 : (k + 1) * 128] = block
        rows = jnp.dot(own_first, table[k, 0], preferred_element_type=F32)
        for i in range(FIRST):
            first[i * BINS + k : i * BINS + k + 1, :] = rows[i : i + 1]
        rows = jnp.dot(own_second, table[k, 1], preferred_element_type=F32).astype(BF16)
        second_sums[k] = jnp.dot(rows, ones, preferred_element_type=F32)
    shape = (GRID, 128)
    wave_first = iota(shape, 0) - CENTRE
    wave_third = iota(shape, 1) % GRID - CENTRE
    quadrant = jnp.where(wave_first * wave_third >= 0, 0, 1)
    own = quadrant == iota(shape, 1) // GRID
    height = jnp.where(own, 16 * jnp.abs(wave_third), 16 * GRID * GRID)
    width = jnp.abs(wave_first)
    rows = first[...].astype(BF16)
    for k in range(SLOPES):
        held = jnp.where(height <= (k + SLOPE_MIN) * width, 1.0, 0.0).astype(BF16)
        grown[:, k * 128 : (k + 1) * 128] = jnp.dot(rows, held, preferred_element_type=F32)


def operators(table):
    return pl.pallas_call(
        operators_kernel,
        out_shape=(
            jax.ShapeDtypeStruct((128, BINS * 128), BF16),
            jax.ShapeDtypeStruct((FIRST * BINS, SLOPES * 128), F32),
            jax.ShapeDtypeStruct((BINS, SECOND, 128), F32),
        ),
        in_specs=[VMEM],
        out_specs=(VMEM,) * 3,
        scratch_shapes=[pltpu.VMEM((FIRST * BINS, GRID), F32)],
        compiler_params=SMALL,
        cost_estimate=pl.CostEstimate(flops=10**8, bytes_accessed=2**20, transcendentals=0),
        name="operators",
    )(table)


def divide_kernel(parts, third, grown, second_sums, out, left):
    total = parts[0]
    for k in range(1, COLS):
        total = total + parts[k]
    counts = total[OWN : OWN + 8]
    low = iota((8, 128), 1) < GRID
    held = [[jnp.zeros((8, 128), F32) for _ in range(2)] for _ in range(FIRST)]
    for k in range(SLOPES):
        for upper in range(2):
            lane = upper * 64 + k
            spread = jnp.where(
                low,
                jnp.broadcast_to(counts[:, lane : lane + 1], (8, 128)),
                jnp.broadcast_to(counts[:, lane + 32 : lane + 33], (8, 128)),
            )
            for i in range(FIRST):
                start = i * BINS + upper * 8
                held[i][upper] += spread * grown[start : start + 8, k * 128 : k * 128 + 128]
    for k in range(BINS):
        sums = second_sums[k]
        for i in range(FIRST):
            value = sums * held[i][k // 8][k % 8 : k % 8 + 1, :]
            upper = value.astype(BF16)
            lower = (value - upper.astype(F32)).astype(BF16)
            lanes = slice(k * 128, k * 128 + 128)
            left[i * SECOND : (i + 1) * SECOND, lanes] = upper.astype(F32)
            left[OWN + i * SECOND : OWN + (i + 1) * SECOND, lanes] = lower.astype(F32)
    weight = lax.dot_general(
        left[...].astype(BF16), third[...], (((1,), (1,)), ((), ())), preferred_element_type=F32
    )
    out[...] = total[0:OWN] / (weight[0:OWN] + weight[OWN:] + 1.0)


def divide(parts, third, grown, second_sums):
    return pl.pallas_call(
        divide_kernel,
        out_shape=jax.ShapeDtypeStruct((OWN, 128), F32),
        in_specs=[VMEM] * 4,
        out_specs=VMEM,
        scratch_shapes=[pltpu.VMEM((2 * OWN, BINS * 128), F32)],
        compiler_params=SMALL,
        name="divide",
    )(parts, third, grown, second_sums)


def spectra_kernel(own, other, out, rows):
    on_first = lax.axis_index("half") == 0
    a, b = own[...], other[...]
    cross = a * b
    own_power, other_power = a * a, b * b
    power_first = jnp.where(on_first, own_power, other_power)
    power_second = jnp.where(on_first, other_power, own_power)
    index = iota((OWN, 128), 0)
    first = index // SECOND + lax.axis_index(ROW) * FIRST - CENTRE
    second = index % SECOND + lax.axis_index("col") * SECOND - CENTRE
    third = iota((OWN, 128), 1) % GRID - CENTRE
    radius_sq = first * first + second * second + third * third
    rows[...] = jnp.zeros_like(rows)
    for k in range(SHELLS):
        least = 0 if k == 0 else (k + 3) ** 2
        inside = (radius_sq >= least) & (radius_sq < (k + 4) ** 2)
        for j, value in enumerate((cross, power_first, power_second)):
            rows[j * 32 + k : j * 32 + k + 1, :] = jnp.sum(
                jnp.where(inside, value, 0.0), axis=0, keepdims=True
            )
    rest = rows[...]
    ones = jnp.ones((8, 128), BF16)
    total = jnp.zeros((8, 128), F32)
    for _ in range(3):
        piece = rest.astype(BF16)
        rest = rest - piece.astype(F32)
        total += lax.dot_general(ones, piece, (((1,), (1,)), ((), ())), preferred_element_type=F32)
    for k in range(COLS):
        out[k] = total[0:1]


def spectra(own, other):
    return pl.pallas_call(
        spectra_kernel,
        out_shape=jax.ShapeDtypeStruct((COLS, 1, 128), F32),
        in_specs=[VMEM, VMEM],
        out_specs=VMEM,
        scratch_shapes=[pltpu.VMEM((128, 128), F32)],
        compiler_params=SMALL,
        name="spectra",
    )(own, other)


def spread_kernel(parts, out):
    total = jnp.sum(parts[...], axis=0)
    for k in range(ROWS):
        out[k] = total


def spread_sum(parts):
    return pl.pallas_call(
        spread_kernel,
        out_shape=jax.ShapeDtypeStruct((ROWS, 1, 128), F32),
        in_specs=[VMEM],
        out_specs=VMEM,
        compiler_params=SMALL,
        name="spread_sum",
    )(parts)


def finish_kernel(parts, own, counts, maps, power, correlation):
    total = jnp.sum(parts[...], axis=0)
    cross = total[0:1, 0:SHELLS]
    first = total[0:1, 32 : 32 + SHELLS]
    second = total[0:1, 64 : 64 + SHELLS]
    power[0:1, :] = first / counts[...]
    power[1:2, :] = second / counts[...]
    correlation[...] = cross / jnp.sqrt(first * second + 1e-06)
    low = iota((SECOND // 2, 128), 1) < GRID
    for i in range(FIRST):
        even = own[pl.ds(i * SECOND, SECOND // 2, stride=2), :]
        odd = own[pl.ds(i * SECOND + 1, SECOND // 2, stride=2), :]
        real = jnp.where(low, even, pltpu.roll(odd, 64, 1))
        imag = jnp.where(low, pltpu.roll(even, 64, 1), odd)
        for j in range(SECOND // 2):
            lanes = slice(j * 128, j * 128 + 128)
            maps[0, 0, i : i + 1, lanes] = real[j : j + 1]
            maps[0, 1, i : i + 1, lanes] = imag[j : j + 1]


def finish(parts, own, counts):
    return pl.pallas_call(
        finish_kernel,
        out_shape=(
            jax.ShapeDtypeStruct((1, 2, FIRST, SECOND * GRID), F32),
            jax.ShapeDtypeStruct((2, SHELLS), F32),
            jax.ShapeDtypeStruct((1, SHELLS), F32),
        ),
        in_specs=[VMEM] * 3,
        out_specs=(VMEM,) * 3,
        compiler_params=SMALL,
        name="finish",
    )(parts, own, counts)


def shifted(shift, swapped=False):
    pairs = []
    for half in range(2):
        for x in range(SIDE):
            for y in range(SIDE):
                along_x = (half == 0) != swapped
                to_x = (x + shift) % SIDE if along_x else x
                to_y = y if along_x else (y + shift) % SIDE
                pairs.append((half * ROWS + x * SIDE + y, half * ROWS + to_x * SIDE + to_y))
    return pairs


def shell_counts():
    wave = np.arange(GRID) - CENTRE
    radius_sq = (wave[:, None, None] ** 2 + wave[None, :, None] ** 2 + wave[None, None, :] ** 2).reshape(-1)
    bounds = np.arange(4, CENTRE) ** 2
    shell = np.searchsorted(bounds, radius_sq, side="right")
    inside = radius_sq < CENTRE * CENTRE
    return np.bincount(shell[inside], minlength=SHELLS).astype(np.float32)[None]


def local(particles, orient_bin, tilt_slope, table):
    inputs = [
        pltpu.with_memory_space_constraint(x, pltpu.HBM)
        for x in (particles, orient_bin, tilt_slope, table)
    ]
    *held, far_low, far_high = first_slab(*inputs)
    far_low = lax.ppermute(far_low, HALF_ROW, shifted(1))
    far_high = lax.ppermute(far_high, HALF_ROW, shifted(3))
    after_high, before_low = direct_slabs(*held)
    after_high = lax.ppermute(after_high, HALF_ROW, shifted(1))
    before_low = lax.ppermute(before_low, HALF_ROW, shifted(3))
    after_low, before_high, own = other_slabs(*held)
    after_low, before_high = add_far(after_low, far_low, before_high, far_high)
    after_low = lax.ppermute(after_low, HALF_ROW, shifted(1))
    before_high = lax.ppermute(before_high, HALF_ROW, shifted(3))
    prepared = operators(table)
    parts = [own, after_low, after_high, before_low, before_high]
    *others, own = gather(*parts)
    parts = [
        lax.ppermute(block, HALF_ROW, shifted(shift, True))
        for shift, block in zip((1, 3, 2), others, strict=True)
    ]
    blocks = reduce(own, *parts)
    parts = lax.all_to_all(blocks, "col", 0, 0, tiled=True)
    own = divide(parts, *prepared)
    other = lax.ppermute(own, "half", [(0, 1), (1, 0)])
    parts = lax.all_to_all(spectra(own, other), "col", 0, 0, tiled=True)
    parts = lax.all_to_all(spread_sum(parts), ROW, 0, 0, tiled=True)
    half_maps, power, correlation = finish(parts, own, jnp.asarray(shell_counts()))
    return half_maps, power, correlation


def solution(mesh):
    torus = Mesh(
        mesh.devices.reshape(mesh.shape["half"], 4, 4, mesh.shape["col"]),
        ("half", "row_0", "row_1", "col"),
    )
    in_specs = (P(HALF_ROW_COL, None, None, None), P(HALF_ROW_COL), P(HALF_ROW_COL, None), P())
    out_specs = (P("half", None, ROW, "col"), P(), P("half", None))
    return jax.shard_map(local, mesh=torus, in_specs=in_specs, out_specs=out_specs, check_vma=False)
```

```python
import jax
import jax.numpy as jnp
import numpy as np
from jax import lax
from jax.experimental import pallas as pl
from jax.experimental.pallas import tpu as pltpu
from jax.sharding import Mesh
from jax.sharding import PartitionSpec as P

SHELLS = 29
GRID = 64
CENTRE = GRID // 2
BINS = 16
ROWS = 16
COLS = 8
FIRST = GRID // ROWS
SECOND = GRID // COLS
SLOPE_MIN = 12
SLOPES = 29
SIDE = 4
PITCH = 68
PIECES = ((0, 4), (4, 12))
BLOCK = FIRST * GRID
OWN = FIRST * SECOND
ROW = ("row_0", "row_1")
HALF_ROW = ("half", "row_0", "row_1")
HALF_ROW_COL = ("half", "row_0", "row_1", "col")
F32 = jnp.float32
BF16 = jnp.bfloat16
VMEM = pl.BlockSpec(memory_space=pltpu.VMEM)
HBM = pl.BlockSpec(memory_space=pltpu.HBM)
SMALL = pltpu.CompilerParams(vmem_limit_bytes=6 * 2**20)


def iota(shape, dim):
    return lax.broadcasted_iota(jnp.int32, shape, dim)


def wedge_tile(slope_first, slope_second):
    wave_first = iota((GRID, 128), 0) - CENTRE
    wave_third = iota((GRID, 128), 1) % GRID - CENTRE
    limit = jnp.where(wave_first * wave_third >= 0, slope_first, slope_second)
    inside = 16 * jnp.abs(wave_third) <= limit * jnp.abs(wave_first)
    return jnp.where(inside, 1.0, 0.0).astype(BF16)


def histogram_tile(bins, slopes):
    row, lane = iota((8, 128), 0), iota((8, 128), 1)
    total = jnp.zeros((8, 128), F32)
    for p in range(2):
        for quadrant in range(2):
            place = (bins[p] // 8) * 64 + quadrant * 32 + slopes[p, quadrant] - SLOPE_MIN
            total += jnp.where((row == bins[p] % 8) & (lane == place), 1.0, 0.0)
    return total


def compute_slab(shift, inners, planes, second, third, out, counts=None):
    on_first = lax.axis_index("half") == 0
    mine = jnp.where(on_first, lax.axis_index("row_0"), lax.axis_index("row_1"))
    outer = lax.rem(mine + shift, SIDE)
    for n, inner in enumerate(inners):
        row = jnp.where(on_first, outer * SIDE + inner, inner * SIDE + outer)
        for i in range(FIRST):
            parts = []
            for p in range(2):
                plane = planes[p, pl.ds(row * FIRST + i, GRID, stride=PITCH), :].astype(BF16)
                along = jnp.dot(second[p], plane, preferred_element_type=F32)
                parts.append(along.astype(BF16))
            full = jnp.dot(jnp.concatenate(parts, axis=1), third[...], preferred_element_type=F32)
            for q in range(COLS):
                start = n * BLOCK + (q * FIRST + i) * SECOND
                out[start : start + SECOND, :] = full[q * SECOND : (q + 1) * SECOND]
    if counts is not None:
        out[len(inners) * BLOCK : len(inners) * BLOCK + 8, :] = counts[...]


LOW = (0, 1)
HIGH = (2, 3)
HALF_SLAB = jax.ShapeDtypeStruct((2 * BLOCK, 128), F32)
HALF_SLAB_COUNTS = jax.ShapeDtypeStruct((2 * BLOCK + 8, 128), F32)
SLAB = jax.ShapeDtypeStruct((SIDE * BLOCK + 8, 128), F32)


def first_kernel(bins_in, slopes_in, particles, table, planes, second, third, counts, far_low, far_high, volume, chosen, bins, slopes, sem):
    scalars = [
        pltpu.make_async_copy(bins_in, bins, sem.at[6]),
        pltpu.make_async_copy(slopes_in, slopes, sem.at[7]),
    ]
    volumes = [
        pltpu.make_async_copy(
            particles.at[:, :, :, pl.ds(start * 256, size * 256)],
            volume.at[:, :, :, pl.ds(start * 256, size * 256)],
            sem.at[k],
        )
        for k, (start, size) in enumerate(PIECES)
    ]
    whole = pltpu.make_async_copy(table, chosen, sem.at[4])
    for copy in (*scalars, whole, *volumes):
        copy.start()
    third[...] = jnp.zeros_like(third)
    low = iota((GRID, 128), 1) < GRID
    for copy in scalars:
        copy.wait()
    wedges = [
        jnp.concatenate([wedge_tile(slopes[p, 0], slopes[p, 1])] * 4, axis=1) for p in range(2)
    ]
    counts[...] = histogram_tile(bins, slopes)
    whole.wait()
    for p in range(2):
        second[p] = chosen[bins[p], 1]
        transposed = chosen[bins[p], 2].astype(F32).T.astype(BF16)
        for c in range(2):
            third[p * 128 + c * 64 : p * 128 + c * 64 + 64, c * 64 : c * 64 + 64] = transposed
    first = [chosen[bins[p], 0] for p in range(2)]

    def transform(chunk):
        for p in range(2):
            tiles = []
            for j in range(2):
                tile = pl.ds(pl.multiple_of(chunk * 256 + j * 128, 128), 128)
                real, imag = (volume[p, c, :, tile] for c in range(2))
                tiles.append(jnp.concatenate([real[:, :GRID], imag[:, :GRID]], axis=1))
                tiles.append(jnp.concatenate([real[:, GRID:], imag[:, GRID:]], axis=1))
            both = jnp.concatenate(tiles, axis=1)
            along = jnp.dot(first[p], both * wedges[p], preferred_element_type=F32)
            for j in range(4):
                base = pl.multiple_of((chunk * 4 + j) * PITCH, 4)
                planes[p, pl.ds(base, GRID), :] = along[:, j * 128 : j * 128 + 128]

    for k, (start, size) in enumerate(PIECES):
        volumes[k].wait()

        @pl.loop(start, start + size, unroll=size)
        def _(chunk):
            transform(chunk)

    compute_slab(2, LOW, planes, second, third, far_low, counts)
    compute_slab(2, HIGH, planes, second, third, far_high)


def first_slab(particles, orient_bin, tilt_slope, table):
    return pl.pallas_call(
        first_kernel,
        out_shape=(
            jax.ShapeDtypeStruct((2, GRID * PITCH, 128), F32),
            jax.ShapeDtypeStruct((2, GRID, GRID), BF16),
            jax.ShapeDtypeStruct((256, 128), BF16),
            jax.ShapeDtypeStruct((8, 128), F32),
            HALF_SLAB_COUNTS,
            HALF_SLAB,
        ),
        in_specs=[HBM] * 4,
        out_specs=(VMEM,) * 6,
        scratch_shapes=[
            pltpu.VMEM((2, 2, GRID, GRID * GRID), BF16),
            pltpu.VMEM((BINS, 3, GRID, GRID), BF16),
            pltpu.SMEM((2,), jnp.int32),
            pltpu.SMEM((2, 2), jnp.int32),
            pltpu.SemaphoreType.DMA((8,)),
        ],
        compiler_params=pltpu.CompilerParams(vmem_limit_bytes=20 * 2**20),
        cost_estimate=pl.CostEstimate(flops=10**9, bytes_accessed=4 * 2**20, transcendentals=0),
        name="first_slab",
    )(orient_bin, tilt_slope, particles, table)


def direct_kernel(planes, second, third, counts, after_high, before_low):
    compute_slab(1, HIGH, planes, second, third, after_high)
    compute_slab(3, LOW, planes, second, third, before_low, counts)


def direct_slabs(planes, second, third, counts):
    return pl.pallas_call(
        direct_kernel,
        out_shape=(HALF_SLAB, HALF_SLAB_COUNTS),
        in_specs=[VMEM] * 4,
        out_specs=(VMEM,) * 2,
        compiler_params=SMALL,
        cost_estimate=pl.CostEstimate(flops=10**9, bytes_accessed=2**20, transcendentals=0),
        name="direct_slabs",
    )(planes, second, third, counts)


def other_kernel(planes, second, third, counts, after_low, before_high, own):
    compute_slab(1, LOW, planes, second, third, after_low, counts)
    compute_slab(3, HIGH, planes, second, third, before_high)
    compute_slab(0, LOW + HIGH, planes, second, third, own, counts)


def other_slabs(planes, second, third, counts):
    return pl.pallas_call(
        other_kernel,
        out_shape=(HALF_SLAB_COUNTS, HALF_SLAB, SLAB),
        in_specs=[VMEM] * 4,
        out_specs=(VMEM,) * 3,
        compiler_params=SMALL,
        cost_estimate=pl.CostEstimate(flops=10**9, bytes_accessed=2**20, transcendentals=0),
        name="other_slabs",
    )(planes, second, third, counts)


def add_kernel(after_low, far_low, before_high, far_high, after_out, before_out):
    after_out[...] = after_low[...] + far_low[...]
    before_out[...] = before_high[...] + far_high[...]


def add_far(after_low, far_low, before_high, far_high):
    return pl.pallas_call(
        add_kernel,
        out_shape=(HALF_SLAB_COUNTS, HALF_SLAB),
        in_specs=[VMEM] * 4,
        out_specs=(VMEM,) * 2,
        compiler_params=SMALL,
        cost_estimate=pl.CostEstimate(flops=10**8, bytes_accessed=2**20, transcendentals=0),
        name="add_far",
    )(after_low, far_low, before_high, far_high)


def gather_kernel(own, after_low, after_high, before_low, before_high, *refs):
    *outs, sums = refs
    on_first = lax.axis_index("half") == 0
    mine = jnp.where(on_first, lax.axis_index("row_1"), lax.axis_index("row_0"))
    half = 2 * BLOCK
    tail = pl.ds(half, 8)
    counts = own[pl.ds(2 * half, 8), :] + after_low[tail, :] + before_low[tail, :]
    for n, parts in enumerate(((after_low, before_low), (after_high, before_high))):
        span = pl.ds(n * half, half)
        sums[span, :] = own[span, :] + parts[0][0:half, :] + parts[1][0:half, :]
    for shift, out in zip((1, 3, 2, 0), outs, strict=True):
        span = pl.ds(pl.multiple_of(lax.rem(mine + shift, SIDE) * BLOCK, 8), BLOCK)
        out[0:BLOCK, :] = sums[span, :]
        out[BLOCK : BLOCK + 8, :] = counts


def gather(*parts):
    return pl.pallas_call(
        gather_kernel,
        out_shape=(jax.ShapeDtypeStruct((BLOCK + 8, 128), F32),) * SIDE,
        in_specs=[VMEM] * len(parts),
        out_specs=(VMEM,) * SIDE,
        scratch_shapes=[pltpu.VMEM((SIDE * BLOCK, 128), F32)],
        compiler_params=SMALL,
        name="gather",
    )(*parts)


def reduce_kernel(*refs):
    *parts, out = refs
    tail = pl.ds(BLOCK, 8)
    counts = parts[0][tail, :]
    for part in parts[1:]:
        counts = counts + part[tail, :]
    for n in range(COLS):
        span = pl.ds(n * OWN, OWN)
        total = parts[0][span, :]
        for part in parts[1:]:
            total = total + part[span, :]
        out[n, 0:OWN, :] = total
        out[n, OWN : OWN + 8, :] = counts


def reduce(*parts):
    return pl.pallas_call(
        reduce_kernel,
        out_shape=jax.ShapeDtypeStruct((COLS, OWN + 8, 128), F32),
        in_specs=[VMEM] * len(parts),
        out_specs=VMEM,
        compiler_params=SMALL,
        name="reduce",
    )(*parts)


def operators_kernel(table, third, grown, second_sums, first):
    row, col = lax.axis_index(ROW), lax.axis_index("col")
    place = iota((8, GRID), 0)
    own_first = (iota((8, GRID), 1) == row * FIRST + place).astype(BF16)
    own_second = (iota((8, GRID), 1) == col * SECOND + place).astype(BF16)
    ones = jnp.ones((GRID, 128), BF16)
    for k in range(BINS):
        block = table[k, 2]
        block = jnp.concatenate([block, block], axis=1)
        for c in range(2):
            third[c * GRID : (c + 1) * GRID, k * 128 : (k + 1) * 128] = block
        rows = jnp.dot(own_first, table[k, 0], preferred_element_type=F32)
        for i in range(FIRST):
            first[i * BINS + k : i * BINS + k + 1, :] = rows[i : i + 1]
        rows = jnp.dot(own_second, table[k, 1], preferred_element_type=F32).astype(BF16)
        second_sums[k] = jnp.dot(rows, ones, preferred_element_type=F32)
    shape = (GRID, 128)
    wave_first = iota(shape, 0) - CENTRE
    wave_third = iota(shape, 1) % GRID - CENTRE
    quadrant = jnp.where(wave_first * wave_third >= 0, 0, 1)
    own = quadrant == iota(shape, 1) // GRID
    height = jnp.where(own, 16 * jnp.abs(wave_third), 16 * GRID * GRID)
    width = jnp.abs(wave_first)
    rows = first[...].astype(BF16)
    for k in range(SLOPES):
        held = jnp.where(height <= (k + SLOPE_MIN) * width, 1.0, 0.0).astype(BF16)
        grown[:, k * 128 : (k + 1) * 128] = jnp.dot(rows, held, preferred_element_type=F32)


def operators(table):
    return pl.pallas_call(
        operators_kernel,
        out_shape=(
            jax.ShapeDtypeStruct((128, BINS * 128), BF16),
            jax.ShapeDtypeStruct((FIRST * BINS, SLOPES * 128), F32),
            jax.ShapeDtypeStruct((BINS, SECOND, 128), F32),
        ),
        in_specs=[VMEM],
        out_specs=(VMEM,) * 3,
        scratch_shapes=[pltpu.VMEM((FIRST * BINS, GRID), F32)],
        compiler_params=SMALL,
        cost_estimate=pl.CostEstimate(flops=10**8, bytes_accessed=2**20, transcendentals=0),
        name="operators",
    )(table)


def divide_kernel(parts, third, grown, second_sums, out, left):
    total = parts[0]
    for k in range(1, COLS):
        total = total + parts[k]
    counts = total[OWN : OWN + 8]
    low = iota((8, 128), 1) < GRID
    held = [[jnp.zeros((8, 128), F32) for _ in range(2)] for _ in range(FIRST)]
    for k in range(SLOPES):
        for upper in range(2):
            lane = upper * 64 + k
            spread = jnp.where(
                low,
                jnp.broadcast_to(counts[:, lane : lane + 1], (8, 128)),
                jnp.broadcast_to(counts[:, lane + 32 : lane + 33], (8, 128)),
            )
            for i in range(FIRST):
                start = i * BINS + upper * 8
                held[i][upper] += spread * grown[start : start + 8, k * 128 : k * 128 + 128]
    for k in range(BINS):
        sums = second_sums[k]
        for i in range(FIRST):
            value = sums * held[i][k // 8][k % 8 : k % 8 + 1, :]
            upper = value.astype(BF16)
            lower = (value - upper.astype(F32)).astype(BF16)
            lanes = slice(k * 128, k * 128 + 128)
            left[i * SECOND : (i + 1) * SECOND, lanes] = upper.astype(F32)
            left[OWN + i * SECOND : OWN + (i + 1) * SECOND, lanes] = lower.astype(F32)
    weight = lax.dot_general(
        left[...].astype(BF16), third[...], (((1,), (1,)), ((), ())), preferred_element_type=F32
    )
    out[...] = total[0:OWN] / (weight[0:OWN] + weight[OWN:] + 1.0)


def divide(parts, third, grown, second_sums):
    return pl.pallas_call(
        divide_kernel,
        out_shape=jax.ShapeDtypeStruct((OWN, 128), F32),
        in_specs=[VMEM] * 4,
        out_specs=VMEM,
        scratch_shapes=[pltpu.VMEM((2 * OWN, BINS * 128), F32)],
        compiler_params=SMALL,
        name="divide",
    )(parts, third, grown, second_sums)


def spectra_kernel(own, other, out, rows):
    on_first = lax.axis_index("half") == 0
    a, b = own[...], other[...]
    cross = a * b
    own_power, other_power = a * a, b * b
    power_first = jnp.where(on_first, own_power, other_power)
    power_second = jnp.where(on_first, other_power, own_power)
    index = iota((OWN, 128), 0)
    first = index // SECOND + lax.axis_index(ROW) * FIRST - CENTRE
    second = index % SECOND + lax.axis_index("col") * SECOND - CENTRE
    third = iota((OWN, 128), 1) % GRID - CENTRE
    radius_sq = first * first + second * second + third * third
    rows[...] = jnp.zeros_like(rows)
    for k in range(SHELLS):
        least = 0 if k == 0 else (k + 3) ** 2
        inside = (radius_sq >= least) & (radius_sq < (k + 4) ** 2)
        for j, value in enumerate((cross, power_first, power_second)):
            rows[j * 32 + k : j * 32 + k + 1, :] = jnp.sum(
                jnp.where(inside, value, 0.0), axis=0, keepdims=True
            )
    rest = rows[...]
    ones = jnp.ones((8, 128), BF16)
    total = jnp.zeros((8, 128), F32)
    for _ in range(3):
        piece = rest.astype(BF16)
        rest = rest - piece.astype(F32)
        total += lax.dot_general(ones, piece, (((1,), (1,)), ((), ())), preferred_element_type=F32)
    for k in range(ROWS):
        out[k] = total[0:1]


def spectra(own, other):
    return pl.pallas_call(
        spectra_kernel,
        out_shape=jax.ShapeDtypeStruct((ROWS, 1, 128), F32),
        in_specs=[VMEM, VMEM],
        out_specs=VMEM,
        scratch_shapes=[pltpu.VMEM((128, 128), F32)],
        compiler_params=SMALL,
        name="spectra",
    )(own, other)


def spread_kernel(parts, out):
    total = jnp.sum(parts[...], axis=0)
    for k in range(COLS):
        out[k] = total


def spread_sum(parts):
    return pl.pallas_call(
        spread_kernel,
        out_shape=jax.ShapeDtypeStruct((COLS, 1, 128), F32),
        in_specs=[VMEM],
        out_specs=VMEM,
        compiler_params=SMALL,
        name="spread_sum",
    )(parts)


def finish_kernel(parts, own, counts, maps, power, correlation):
    total = jnp.sum(parts[...], axis=0)
    cross = total[0:1, 0:SHELLS]
    first = total[0:1, 32 : 32 + SHELLS]
    second = total[0:1, 64 : 64 + SHELLS]
    power[0:1, :] = first / counts[...]
    power[1:2, :] = second / counts[...]
    correlation[...] = cross / jnp.sqrt(first * second + 1e-06)
    low = iota((SECOND // 2, 128), 1) < GRID
    for i in range(FIRST):
        even = own[pl.ds(i * SECOND, SECOND // 2, stride=2), :]
        odd = own[pl.ds(i * SECOND + 1, SECOND // 2, stride=2), :]
        real = jnp.where(low, even, pltpu.roll(odd, 64, 1))
        imag = jnp.where(low, pltpu.roll(even, 64, 1), odd)
        for j in range(SECOND // 2):
            lanes = slice(j * 128, j * 128 + 128)
            maps[0, 0, i : i + 1, lanes] = real[j : j + 1]
            maps[0, 1, i : i + 1, lanes] = imag[j : j + 1]


def finish(parts, own, counts):
    return pl.pallas_call(
        finish_kernel,
        out_shape=(
            jax.ShapeDtypeStruct((1, 2, FIRST, SECOND * GRID), F32),
            jax.ShapeDtypeStruct((2, SHELLS), F32),
            jax.ShapeDtypeStruct((1, SHELLS), F32),
        ),
        in_specs=[VMEM] * 3,
        out_specs=(VMEM,) * 3,
        compiler_params=SMALL,
        name="finish",
    )(parts, own, counts)


def shifted(shift, swapped=False):
    pairs = []
    for half in range(2):
        for x in range(SIDE):
            for y in range(SIDE):
                along_x = (half == 0) != swapped
                to_x = (x + shift) % SIDE if along_x else x
                to_y = y if along_x else (y + shift) % SIDE
                pairs.append((half * ROWS + x * SIDE + y, half * ROWS + to_x * SIDE + to_y))
    return pairs


def shell_counts():
    wave = np.arange(GRID) - CENTRE
    radius_sq = (wave[:, None, None] ** 2 + wave[None, :, None] ** 2 + wave[None, None, :] ** 2).reshape(-1)
    bounds = np.arange(4, CENTRE) ** 2
    shell = np.searchsorted(bounds, radius_sq, side="right")
    inside = radius_sq < CENTRE * CENTRE
    return np.bincount(shell[inside], minlength=SHELLS).astype(np.float32)[None]


def local(particles, orient_bin, tilt_slope, table):
    inputs = [
        pltpu.with_memory_space_constraint(x, pltpu.HBM)
        for x in (particles, orient_bin, tilt_slope, table)
    ]
    *held, far_low, far_high = first_slab(*inputs)
    far_low = lax.ppermute(far_low, HALF_ROW, shifted(1))
    far_high = lax.ppermute(far_high, HALF_ROW, shifted(3))
    after_high, before_low = direct_slabs(*held)
    after_high = lax.ppermute(after_high, HALF_ROW, shifted(1))
    before_low = lax.ppermute(before_low, HALF_ROW, shifted(3))
    after_low, before_high, own = other_slabs(*held)
    after_low, before_high = add_far(after_low, far_low, before_high, far_high)
    after_low = lax.ppermute(after_low, HALF_ROW, shifted(1))
    before_high = lax.ppermute(before_high, HALF_ROW, shifted(3))
    prepared = operators(table)
    parts = [own, after_low, after_high, before_low, before_high]
    *others, own = gather(*parts)
    parts = [
        lax.ppermute(block, HALF_ROW, shifted(shift, True))
        for shift, block in zip((1, 3, 2), others, strict=True)
    ]
    blocks = reduce(own, *parts)
    parts = lax.all_to_all(blocks, "col", 0, 0, tiled=True)
    own = divide(parts, *prepared)
    other = lax.ppermute(own, "half", [(0, 1), (1, 0)])
    parts = lax.all_to_all(spectra(own, other), ROW, 0, 0, tiled=True)
    parts = lax.all_to_all(spread_sum(parts), "col", 0, 0, tiled=True)
    half_maps, power, correlation = finish(parts, own, jnp.asarray(shell_counts()))
    return half_maps, power, correlation


def solution(mesh):
    torus = Mesh(
        mesh.devices.reshape(mesh.shape["half"], 4, 4, mesh.shape["col"]),
        ("half", "row_0", "row_1", "col"),
    )
    in_specs = (P(HALF_ROW_COL, None, None, None), P(HALF_ROW_COL), P(HALF_ROW_COL, None), P())
    out_specs = (P("half", None, ROW, "col"), P(), P("half", None))
    return jax.shard_map(local, mesh=torus, in_specs=in_specs, out_specs=out_specs, check_vma=False)
```
